256 devices in a mesh: seq: 8 (over x, core), dom: 32 (over z, y).
Axes of the slice: x: 4, y: 4, z: 8, core: 2. Of those that a mesh axis runs over, the one named last changes fastest.
Arguments:
- observed: bfloat16 [40, 88], P('seq'), parts along dimension 0, may hold values from -18 to 18
- latent_noise: float32 [4, 128, 32768], P(None, None, ('seq', 'dom')), parts along dimension 2, may hold values from -6 to 6
- w_hidden: bfloat16 [4096, 1024], replicated, may hold values from -0.1875 to 0.1875
- w_latent: bfloat16 [4096, 128], replicated, may hold values from -0.5 to 0.5
- w_frame: bfloat16 [88, 4096], replicated, may hold values from -0.625 to 0.625
- gate_bias: float32 [4096], replicated, may hold values from -3 to 3
- w_prior: bfloat16 [256, 1024], replicated, may hold values from -0.1875 to 0.1875
- w_emit: bfloat16 [88, 128], replicated, may hold values from -0.09375 to 0.09375
- w_emit_hidden: bfloat16 [88, 1024], replicated, may hold values from -0.046875 to 0.046875
- block_source: int32 [24, 32], P('seq'), parts along dimension 0, may hold values from 0 to 31, as said below
- inner_offset: int32 [24, 4096], P('seq'), parts along dimension 0, may hold values from 0 to 127
- resample_flags: int32 [3], replicated, may hold values from 0 to 1, as said below
Outputs:
- final_hidden: bfloat16 [1024, 32768], P(None, ('seq', 'dom')), parts along dimension 1
- fivo_bound: float32 [8], P('seq'), parts along dimension 0
The draws below stay inside these ranges and needn't reach their ends.
There are 8 independent parts, one for each index of `seq`. The reference program is written for one: setup_inputs(seed, part) draws one part's arguments, and reference() takes and returns one part's arrays. A program takes and returns all parts, laid end to end along the dimension named above; an argument that names none is the same for every part. Nothing has to cross between parts.
Inputs may be any that keep to these rules, and one draw needn't show every extreme that they name: block_source[t, j] differs from j by at most 1 for every transition t and block j; in every draw some block takes the particles of the block 1 places before it and some those of the block 1 places after it. `resample_flags`: at least one entry is 1 and at least one is 0.
All inputs are finite; a program needn't handle non-finite values.
Results may differ from the reference program's by a relative error of at most 0.0023.
The reference program's roundings to bfloat16 on the way (of `hidden`, `cell_state` and `latent`) count: a program that leaves them out, or rounds other values in their place, can miss the bound.
Values may be sent and summed in bfloat16 or wider, within the bound.
A program may use at most 64 MiB of HBM per device.

```python
import math
import jax
import jax.numpy as jnp

H = 1024
Z = 128
X = 88
BLK = 128
REACH = 1
NB_DEV = 1
STEPS = 4
RESAMPLES = 3
NBLK = 32
NPART = 4096


def draw_observed(key, part):
    key_rows, key_signs = jax.random.split(key)
    frame_rows = jnp.clip(0.8 * jax.random.normal(key_rows, (STEPS + 1, X), jnp.float32), -4.8, 4.8)
    return frame_rows.astype(jnp.bfloat16)


def draw_latent_noise(key, part):
    values = jnp.clip(jax.random.normal(key, (STEPS, Z, NPART), jnp.float32), -6.0, 6.0)
    return values


def draw_block_source(key, part):
    shifts = jax.random.randint(key, (RESAMPLES, NBLK), -REACH, REACH + 1)
    shifts = shifts.at[:, NB_DEV].set(-REACH)
    shifts = shifts.at[:, 3 * NB_DEV - 1].set(REACH)
    places = jnp.arange(NBLK, dtype=jnp.int32)[None, :] + shifts
    return jnp.clip(places, 0, NBLK - 1).astype(jnp.int32)


def draw_resample_flags(key, part):
    key_bits, key_one, key_zero = jax.random.split(key, 3)
    chosen = jax.random.randint(key_bits, (RESAMPLES,), 0, 2)
    ones_at = jax.random.randint(key_one, (), 0, RESAMPLES)
    zero_at = (ones_at + 1 + jax.random.randint(key_zero, (), 0, RESAMPLES - 1)) % RESAMPLES
    chosen = chosen.at[ones_at].set(1).at[zero_at].set(0)
    return chosen.astype(jnp.int32)


def plant(array, own_key, least, high):
    index_at = [jax.random.randint(jax.random.fold_in(own_key, axis), (), 0, length) for axis, length in enumerate(array.shape)]
    main_axis = array.shape.index(max(array.shape))
    neighbour = index_at[:main_axis] + [(index_at[main_axis] + 1) % array.shape[main_axis]] + index_at[main_axis + 1:]
    return array.at[tuple(index_at)].set(least).at[tuple(neighbour)].set(high)


def noise(own_key, dims, scale, bound, kind=jnp.bfloat16):
    drawn = scale * jax.random.normal(own_key, dims, jnp.float32)
    return jnp.clip(drawn, min=-bound, max=bound).astype(kind)


def setup_inputs(seed: int = 0, part: int = 0) -> dict:
    streams_of = jax.random.split(jax.random.key(seed), 13)
    own_keys = jax.random.split(jax.random.fold_in(streams_of[12], part), 13)
    return {
        "observed": draw_observed(jax.random.fold_in(jax.random.fold_in(streams_of[12], part), 71), part),
        "latent_noise": draw_latent_noise(jax.random.fold_in(jax.random.fold_in(streams_of[12], part), 71), part),
        "w_hidden": noise(streams_of[2], (4 * H, H), H ** -0.5, 0.1875),
        "w_latent": noise(streams_of[3], (4 * H, Z), Z ** -0.5, 0.5),
        "w_frame": noise(streams_of[4], (X, 4 * H), X ** -0.5, 0.625),
        "gate_bias": noise(streams_of[5], (4 * H,), 0.5, 3.0, jnp.float32),
        "w_prior": noise(streams_of[6], (2 * Z, H), H ** -0.5, 0.1875),
        "w_emit": noise(streams_of[7], (X, Z), (32 * Z) ** -0.5, 0.09375),
        "w_emit_hidden": noise(streams_of[8], (X, H), (16 * H) ** -0.5, 0.046875),
        "block_source": draw_block_source(jax.random.fold_in(jax.random.fold_in(streams_of[12], part), 71), part),
        "inner_offset": plant(jax.random.randint(own_keys[10], (RESAMPLES, NPART), 0, BLK), jax.random.fold_in(own_keys[10], 1), 0, BLK - 1).astype(jnp.int32),
        "resample_flags": draw_resample_flags(jax.random.fold_in(streams_of[12], 71), part),
    }


def cell_update(gate_pre, cell_state, width):
    in_gate = jax.nn.sigmoid(gate_pre[:width])
    forget = jax.nn.sigmoid(gate_pre[width:2 * width])
    cand_gate = jnp.tanh(gate_pre[2 * width:3 * width])
    out_gate = jax.nn.sigmoid(gate_pre[3 * width:])
    fresh = forget * cell_state.astype(jnp.float32) + in_gate * cand_gate
    hidden = (out_gate * jnp.tanh(fresh)).astype(jnp.bfloat16)
    return hidden, fresh.astype(jnp.bfloat16)


def particle_step(hidden, latent, cell_state, frame_row, moment_noise, target_row, w_hidden, w_latent, gate_bias, w_prior, w_emit, w_emit_hidden):
    gate_pre = jnp.dot(w_hidden, hidden, preferred_element_type=jnp.float32)
    gate_pre = gate_pre + jnp.dot(w_latent, latent, preferred_element_type=jnp.float32)
    gate_pre = gate_pre + (frame_row + gate_bias)[:, None]
    hidden, cell_state = cell_update(gate_pre, cell_state, w_hidden.shape[1])
    prior_out = jnp.dot(w_prior, hidden, preferred_element_type=jnp.float32)
    zdim = w_latent.shape[1]
    latent = (prior_out[:zdim] + jnp.exp(0.5 * jnp.tanh(prior_out[zdim:])) * moment_noise).astype(jnp.bfloat16)
    predicted = jnp.dot(w_emit, latent, preferred_element_type=jnp.float32)
    predicted = predicted + jnp.dot(w_emit_hidden, hidden, preferred_element_type=jnp.float32)
    target = target_row.astype(jnp.float32)[:, None]
    increment = jnp.sum(predicted * (target - 0.5 * predicted), axis=0)
    return hidden, latent, cell_state, increment


def reference(observed, latent_noise, w_hidden, w_latent, w_frame, gate_bias, w_prior, w_emit, w_emit_hidden, block_source, inner_offset, resample_flags):
    width = w_hidden.shape[1]
    zdim = w_latent.shape[1]
    particles = latent_noise.shape[2]
    frames = jnp.dot(observed[:STEPS], w_frame, preferred_element_type=jnp.float32)
    hidden = jnp.zeros((width, particles), jnp.bfloat16)
    cell_state = jnp.zeros((width, particles), jnp.bfloat16)
    latent = jnp.zeros((zdim, particles), jnp.bfloat16)
    log_weight = jnp.zeros((particles,), jnp.float32)
    bound_sum = jnp.zeros((), jnp.float32)
    log_count = math.log(particles)
    for moment in range(STEPS):
        hidden, latent, cell_state, increment = particle_step(hidden, latent, cell_state, frames[moment], latent_noise[moment], observed[moment + 1], w_hidden, w_latent, gate_bias, w_prior, w_emit, w_emit_hidden)
        log_weight = log_weight + increment
        if moment < STEPS - 1:
            do_move = resample_flags[moment] == 1
            level_now = jax.nn.logsumexp(log_weight) - log_count
            bound_sum = bound_sum + jnp.where(do_move, level_now, jnp.zeros_like(level_now))
            ancestor = (block_source[moment][:, None] * BLK + inner_offset[moment].reshape(-1, BLK)).reshape(-1).astype(jnp.int32)
            hidden = jnp.where(do_move, hidden[:, ancestor], hidden)
            latent = jnp.where(do_move, latent[:, ancestor], latent)
            cell_state = jnp.where(do_move, cell_state[:, ancestor], cell_state)
            log_weight = jnp.where(do_move, jnp.zeros_like(log_weight), log_weight)
    bound_sum = bound_sum + jax.nn.logsumexp(log_weight) - log_count
    return hidden, bound_sum.reshape(1)
```

```python
import functools
import math

import jax
import jax.numpy as jnp
from jax import lax
from jax.experimental import pallas as pl
from jax.experimental.pallas import tpu as pltpu
from jax.sharding import PartitionSpec as P

BLK = 128
F32 = jnp.float32
BF16 = jnp.bfloat16
MESH = pl.DeviceIdType.MESH
CH = 4


def mm(a, b):
    return jnp.dot(a, b, preferred_element_type=F32)


def sig(x):
    return 0.5 * jnp.tanh(0.5 * x) + 0.5


def cell_update(gates, old, n):
    in_gate = sig(gates[:n])
    forget = sig(gates[n : 2 * n])
    cand = jnp.tanh(gates[2 * n : 3 * n])
    out_gate = sig(gates[3 * n :])
    fresh = forget * old.astype(F32) + in_gate * cand
    return (out_gate * jnp.tanh(fresh)).astype(BF16), fresh.astype(BF16)


def split3(x):
    hi = x.astype(BF16)
    rest = x - hi.astype(F32)
    mid = rest.astype(BF16)
    return hi, mid, (rest - mid.astype(F32)).astype(BF16)


def kernel(
    D,
    obs_h,
    nz_h,
    wh_h,
    wl_h,
    wf_h,
    bias_h,
    wp_h,
    we_h,
    weh_h,
    bs_h,
    off_h,
    fl_h,
    hid_o,
    bnd_o,
    wh,
    wlf,
    wf,
    tpose,
    bias,
    wp,
    we,
    weh,
    obs,
    obs_pad,
    nz,
    off,
    bs,
    fl,
    from_l,
    from_r,
    x0,
    x0_l,
    x0_r,
    x1,
    x1_l,
    x1_r,
    g1,
    ga,
    gb,
    hz,
    cz,
    h1,
    c1,
    hc,
    cc,
    h2,
    c2,
    h3,
    c3,
    h4,
    lse_row,
    lse_all,
    wsem,
    lsem,
    osem,
    ssem,
    rsem,
    as_sem,
    ar_sem,
    near_sem,
):
    H = wh.shape[2]
    Z = we.shape[1]
    X = we.shape[0]
    HC = H // CH
    me = lax.axis_index("dom")
    right = lax.rem(me + 1, D)
    left = lax.rem(me + D - 1, D)

    barrier = pltpu.get_barrier_semaphore()
    for nb in (left, right):
        pl.semaphore_signal(barrier, inc=1, device_id={"dom": nb}, device_id_type=MESH)

    small = []

    def fetch(src, dst):
        cp = pltpu.make_async_copy(src, dst, lsem.at[len(small)])
        cp.start()
        small.append(cp)
        return cp

    cp_nz = [fetch(nz_h.at[t], nz.at[t]) for t in range(2)]
    cp_bs = fetch(bs_h, bs)
    cp_fl = fetch(fl_h, fl)
    cp_wf = fetch(wf_h, wf)
    cp_bias = fetch(bias_h, bias)
    cp_obs = fetch(obs_h, obs)
    cp_off = fetch(off_h, off)

    def weight_copies(c):
        res = []
        for g in range(4):
            rows = pl.ds(g * H + c * HC, HC)
            res.append(
                pltpu.make_async_copy(
                    wh_h.at[rows, :], wh.at[c, pl.ds(g * HC, HC), :], wsem.at[0, c, g]
                )
            )
            res.append(
                pltpu.make_async_copy(
                    wl_h.at[rows, :], wlf.at[c, pl.ds(g * HC, HC), pl.ds(0, Z)], wsem.at[1, c, g]
                )
            )
        return res

    wcp = [weight_copies(c) for c in range(CH)]
    for cp in wcp[0]:
        cp.start()
    cp_wp = fetch(wp_h, wp)
    cp_nz += [fetch(nz_h.at[t], nz.at[t]) for t in range(2, 4)]
    cp_we = fetch(we_h, we)
    cp_weh = fetch(weh_h, weh)
    for c in range(1, CH):
        for cp in wcp[c]:
            cp.start()

    def send(k, src, to_right_dst, to_left_dst):
        res = []
        for side, (dst, dev) in enumerate(((to_right_dst, right), (to_left_dst, left))):
            cp = pltpu.make_async_remote_copy(
                src_ref=src,
                dst_ref=dst,
                send_sem=ssem.at[side, k],
                recv_sem=rsem.at[side, k],
                device_id={"dom": dev},
                device_id_type=MESH,
            )
            cp.start()
            res.append(cp)
        return res

    hz[...] = jnp.zeros_like(hz)
    cz[...] = jnp.zeros_like(cz)
    obs_pad[...] = jnp.zeros_like(obs_pad)
    tpose[X // 16 * 16 :, :] = jnp.zeros((BLK - X // 16 * 16, tpose.shape[1]), BF16)

    cp_nz[0].wait()
    cp_nz[1].wait()
    pl.semaphore_wait(barrier, 2)
    sent = []
    for t in range(2):
        sent += [send(t, nz.at[t], from_l.at[t], from_r.at[t])]

    cp_bs.wait()
    cp_fl.wait()
    cp_off.wait()
    cp_obs.wait()
    f0, f1, f2 = fl[0] == 1, fl[1] == 1, fl[2] == 1

    around = range(-2, 3)
    place = [lax.rem(me + d + D, D) for d in around]

    def src(t, k, f):
        found = bs[t, place[2]]
        for d, p in zip(around, place):
            found = jnp.where(k - me == d, bs[t, p], found)
        return jnp.where(f, found, k)

    lane = lax.broadcasted_iota(jnp.int32, (1, BLK), 1).astype(F32)
    sub_i = lax.broadcasted_iota(jnp.int32, (BLK, BLK), 0)
    sub = sub_i.astype(F32)

    def flag_mask(f, shape):
        return jnp.broadcast_to(f.astype(jnp.int32), shape) > 0

    def offs(t, k, f):
        away = jnp.broadcast_to(k - me, (1, BLK))
        row = lane
        for d, p in zip(around, place):
            there = off[pl.ds(t, 1), pl.ds(pl.multiple_of(p * BLK, BLK), BLK)].astype(F32)
            row = jnp.where(jnp.logical_and(flag_mask(f, (1, BLK)), away == d), there, row)
        return row

    def onehot(row):
        return jnp.where(sub == row, 1.0, 0.0).astype(BF16)

    def comp(row, hot):
        return mm(jnp.broadcast_to(row, (16, BLK)).astype(BF16), hot)[:1]

    k2 = src(2, me, f2)
    k1 = src(1, k2, f1)
    s1 = src(1, me, f1)
    s0 = src(0, me, f0)
    both = jnp.logical_and(f0, f1)
    hot_q = onehot(offs(2, me, f2))
    hot_r = onehot(comp(offs(1, k2, f1), hot_q))
    hot_s = onehot(comp(offs(0, k1, f0), hot_r))
    hot_o1 = onehot(offs(1, me, f1))
    hot_o0 = onehot(comp(offs(0, s1, f0), hot_o1))
    hot_c0 = onehot(offs(0, me, f0))
    x0_src = jnp.where(f0, s0, s1)
    hop_o = jnp.where(both, s1, me)
    hop_l = jnp.where(f2, k2, hop_o)

    def pick(a, b, c, k):
        d = jnp.broadcast_to(k - me, a.shape)
        return jnp.where(d < 0, a, jnp.where(d > 0, c, b))

    def gather3(x, hot):
        hi, mid, lo = split3(x)
        out = mm(jnp.concatenate([hi, mid, lo], axis=0), hot)
        return out[:BLK] + out[BLK : 2 * BLK] + out[2 * BLK :]

    steps = obs.shape[0] - 1
    obs_pad[0 : steps + 1, 0:X] = obs[...].astype(F32)
    obs_t = jnp.transpose(obs_pad[...])

    def frame_col(t):
        return jnp.broadcast_to(obs_t[:, t : t + 1], (BLK, BLK))

    ones = jnp.logical_and(sub_i >= 96, sub_i < 99)
    tails = [jnp.where(ones, 1.0, frame_col(t)).astype(BF16) for t in range(steps)]

    cp_wf.wait()
    cp_bias.wait()
    tpose[0:X, :] = wf[...]
    hi, mid, lo = (p.astype(F32) for p in split3(bias[...]))
    r16 = lax.broadcasted_iota(jnp.int32, (16, bias.shape[1]), 0)
    tpose[96:112, :] = jnp.where(
        r16 == 0, hi, jnp.where(r16 == 1, mid, jnp.where(r16 == 2, lo, 0.0))
    ).astype(BF16)
    for c in range(CH):
        for g in range(4):
            for i in range(0, HC, BLK):
                rows = g * H + c * HC + i
                wlf[c, g * HC + i : g * HC + i + BLK, Z : Z + BLK] = jnp.transpose(
                    tpose[:, rows : rows + BLK]
                )

    def run_layer(gates, elem):
        bufs = (ga, gb)
        for c in range(CH):
            val = gates(c)
            bufs[c % 2][:, : val.shape[1]] = val
            if c:
                elem(c - 1, bufs[(c - 1) % 2])
        elem(CH - 1, bufs[(CH - 1) % 2])

    def elem_of(n, old, h_out, c_out):
        def elem(c, buf):
            rows = slice(c * HC, (c + 1) * HC)
            h, s = cell_update(buf[:, :n], old[rows, :n], HC)
            h_out[rows, :n] = h
            if c_out is not None:
                c_out[rows, :n] = s

        return elem

    def moments(h):
        p = mm(wp[...], h)
        return p[:Z], jnp.exp(0.5 * jnp.tanh(p[Z:]))

    def increment(t, lat, h):
        pred = mm(we[...], lat) + mm(weh[...], h)
        target = frame_col(t + 1)[:X]
        return jnp.sum(pred * (target - 0.5 * pred), axis=0, keepdims=True)

    lat_tail0 = jnp.concatenate([jnp.zeros((Z, BLK), BF16), tails[0]], axis=0)

    def gates0(c):
        for cp in wcp[c]:
            cp.wait()
        return mm(wh[c], hz[...]) + mm(wlf[c], lat_tail0)

    run_layer(gates0, elem_of(BLK, cz, h1, c1))
    cp_wp.wait()
    mean0, std0 = moments(h1[...])
    cp_we.wait()
    cp_weh.wait()
    lw0 = increment(0, (mean0 + std0 * nz[0]).astype(BF16), h1[...])

    for c in range(CH // 2):
        g1[c] = mm(wh[c], h1[...])

    def near(i, dist):
        for dev in (lax.rem(me + dist, D), lax.rem(me + D - dist, D)):
            pl.semaphore_signal(
                near_sem.at[i], inc=1, device_id={"dom": dev}, device_id_type=MESH
            )

    near(0, 1)

    def arrived(k, bufs):
        for cp in bufs[k]:
            cp.wait_recv()

    arrived(0, sent)
    n0 = pick(from_l[0], nz[0], from_r[0], x0_src)
    x0[...] = (mean0 + std0 * n0).astype(BF16)
    arrived(1, sent)
    x1[...] = pick(from_l[1], nz[1], from_r[1], s1)
    for c in range(CH // 2, CH):
        g1[c] = mm(wh[c], h1[...])
    sent += [send(2, x0, x0_l, x0_r)]
    sent += [send(3, x1, x1_l, x1_r)]
    cp_nz[2].wait()
    cp_nz[3].wait()
    sent += [send(4, nz.at[2], from_l.at[2], from_r.at[2])]
    pl.semaphore_wait(near_sem.at[0], 2)
    dist, count = 2, 1
    waits = []
    while dist < D // 2:
        waits.append((count, dist))
        dist, count = dist * 2, count + 1

    lat_c = mm(
        (mean0 + std0 * pick(from_l[0], nz[0], from_r[0], s0)).astype(BF16), hot_c0
    ).astype(BF16)
    tail_c = jnp.concatenate([lat_c, tails[1]], axis=0)
    run_layer(lambda c: g1[c] + mm(wlf[c], tail_c), elem_of(BLK, c1, hc, None))
    mean_c, std_c = moments(hc[...])
    inc_c = increment(1, (mean_c + std_c * nz[1]).astype(BF16), hc[...])
    lw1 = jnp.where(flag_mask(f0, (1, BLK)), 0.0, lw0) + inc_c

    for i, d in waits[:1]:
        near(i, d)
    arrived(2, sent)
    x0s = (x0_l[...].astype(F32), x0[...].astype(F32), x0_r[...].astype(F32))
    lat_o = mm(pick(*x0s, hop_o).astype(BF16), hot_o0).astype(BF16)
    lat_l = mm(pick(*x0s, hop_l).astype(BF16), hot_s).astype(BF16)
    tail_ol = jnp.concatenate(
        [
            jnp.concatenate([lat_o, lat_l], axis=1),
            jnp.concatenate([tails[1], tails[1]], axis=1),
        ],
        axis=0,
    )

    def gates1(c):
        g = g1[c]
        return jnp.concatenate([g, g], axis=1) + mm(wlf[c], tail_ol)

    def elem1(c, buf):
        rows = slice(c * HC, (c + 1) * HC)
        old = c1[rows, :]
        h, s = cell_update(buf[...], jnp.concatenate([old, old], axis=1), HC)
        h2[rows, :] = h
        c2[rows, :] = s

    run_layer(gates1, elem1)
    for i, d in waits[:1]:
        pl.semaphore_wait(near_sem.at[i], 2)
    for i, d in waits[1:2]:
        near(i, d)
    m1, sd1 = moments(h2[...])
    arrived(3, sent)
    n1_o = gather3(x1[...], hot_o1)
    n1_l = gather3(pick(x1_l[...], x1[...], x1_r[...], k2), hot_r)
    lat1 = (m1 + sd1 * jnp.concatenate([n1_o, n1_l], axis=1)).astype(BF16)

    tail2 = jnp.concatenate(
        [lat1, jnp.concatenate([tails[2], tails[2]], axis=1)], axis=0
    )
    run_layer(
        lambda c: mm(wh[c], h2[...]) + mm(wlf[c], tail2), elem_of(2 * BLK, c2, h3, c3)
    )
    for i, d in waits[1:2]:
        pl.semaphore_wait(near_sem.at[i], 2)
    for i, d in waits[2:3]:
        near(i, d)
    m2, sd2 = moments(h3[...])
    arrived(4, sent)
    n2_l = gather3(pick(from_l[2], nz[2], from_r[2], k2), hot_q)
    lat2 = (m2 + sd2 * jnp.concatenate([nz[2], n2_l], axis=1)).astype(BF16)
    inc2 = increment(2, lat2[:, :BLK], h3[:, :BLK])
    lw2 = jnp.where(flag_mask(f1, (1, BLK)), 0.0, lw1) + inc2

    tail3 = jnp.concatenate([lat2[:, BLK:], tails[3]], axis=0)

    def gates3(c):
        return mm(wh[c], h3[:, BLK:]) + mm(wlf[c], tail3)

    def elem3(c, buf):
        rows = slice(c * HC, (c + 1) * HC)
        h, _ = cell_update(buf[:, :BLK], c3[rows, BLK:], HC)
        h4[rows, :] = h

    run_layer(gates3, elem3)
    out_cp = pltpu.make_async_copy(h4, hid_o, osem)
    out_cp.start()
    for i, d in waits[2:3]:
        pl.semaphore_wait(near_sem.at[i], 2)
    m3, sd3 = moments(h4[...])
    lat3 = (m3 + sd3 * nz[3]).astype(BF16)
    lw3 = jnp.where(flag_mask(f2, (1, BLK)), 0.0, lw2) + increment(3, lat3, h4[...])

    def lse(lw):
        peak = jnp.max(lw, axis=1, keepdims=True)
        return peak + jnp.log(jnp.sum(jnp.exp(lw - peak), axis=1, keepdims=True))

    lane_i = lax.broadcasted_iota(jnp.int32, (1, BLK), 1)
    row = jnp.zeros((1, BLK), F32)
    for t, lw in enumerate((lw0, lw1, lw2, lw3)):
        row = jnp.where(lane_i == t, lse(lw), row)
    lse_row[...] = row
    lse_all[pl.ds(me, 1)] = row[None]
    pushes = []
    for d in range(1, D):
        dev = lax.rem(me + d, D)
        cp = pltpu.make_async_remote_copy(
            src_ref=lse_row,
            dst_ref=lse_all.at[me],
            send_sem=as_sem.at[d],
            recv_sem=ar_sem.at[me],
            device_id={"dom": dev},
            device_id_type=MESH,
        )
        cp.start()
        pushes.append(cp)
    for two in sent:
        for cp in two:
            cp.wait_send()
    out_cp.wait()
    for d in range(1, D):
        frm = lax.rem(me + d, D)
        pltpu.make_async_remote_copy(
            src_ref=lse_row,
            dst_ref=lse_all.at[frm],
            send_sem=as_sem.at[d],
            recv_sem=ar_sem.at[frm],
            device_id={"dom": frm},
            device_id_type=MESH,
        ).wait_recv()
    for cp in pushes:
        cp.wait_send()
    every = lse_all[...]
    peak = jnp.max(every, axis=0)
    level = peak + jnp.log(jnp.sum(jnp.exp(every - peak[None]), axis=0)) - math.log(D * BLK)
    used = lane_i == steps - 1
    for t, f in enumerate((f0, f1, f2)):
        used = jnp.logical_or(used, jnp.logical_and(lane_i == t, flag_mask(f, (1, BLK))))
    bnd_o[...] = jnp.sum(jnp.where(used, level, 0.0), axis=1, keepdims=True)


def body(
    observed,
    latent_noise,
    w_hidden,
    w_latent,
    w_frame,
    gate_bias,
    w_prior,
    w_emit,
    w_emit_hidden,
    block_source,
    inner_offset,
    resample_flags,
):
    D = lax.axis_size("dom")
    steps, Z, n = latent_noise.shape
    H = w_hidden.shape[1]
    X = w_emit.shape[0]
    G = 4 * H // CH
    V = pltpu.VMEM
    DMA = pltpu.SemaphoreType.DMA
    hidden, bound = pl.pallas_call(
        functools.partial(kernel, D),
        out_shape=(
            jax.ShapeDtypeStruct((H, n), BF16),
            jax.ShapeDtypeStruct((1, 1), F32),
        ),
        in_specs=[pl.BlockSpec(memory_space=pl.ANY)] * 12,
        out_specs=(
            pl.BlockSpec(memory_space=pl.ANY),
            pl.BlockSpec(memory_space=pltpu.VMEM),
        ),
        scratch_shapes=[
            V((CH, G, H), BF16),
            V((CH, G, Z + BLK), BF16),
            V((X, 4 * H), BF16),
            V((BLK, 4 * H), BF16),
            V((1, 4 * H), F32),
            V((2 * Z, H), BF16),
            V((X, Z), BF16),
            V((X, H), BF16),
            V((steps + 1, X), BF16),
            V((BLK, BLK), F32),
            V((steps, Z, n), F32),
            V(inner_offset.shape, jnp.int32),
            pltpu.SMEM(block_source.shape, jnp.int32),
            pltpu.SMEM(resample_flags.shape, jnp.int32),
            V((3, Z, n), F32),
            V((3, Z, n), F32),
            V((Z, n), BF16),
            V((Z, n), BF16),
            V((Z, n), BF16),
            V((Z, n), F32),
            V((Z, n), F32),
            V((Z, n), F32),
            V((CH, G, n), F32),
            V((G, 2 * n), F32),
            V((G, 2 * n), F32),
            V((H, n), BF16),
            V((H, n), BF16),
            V((H, n), BF16),
            V((H, n), BF16),
            V((H, n), BF16),
            V((H, n), BF16),
            V((H, 2 * n), BF16),
            V((H, 2 * n), BF16),
            V((H, 2 * n), BF16),
            V((H, 2 * n), BF16),
            V((H, n), BF16),
            V((1, BLK), F32),
            V((D, 1, BLK), F32),
            DMA((2, CH, 4)),
            DMA((16,)),
            DMA,
            DMA((2, 5)),
            DMA((2, 5)),
            DMA((D,)),
            DMA((D,)),
            pltpu.SemaphoreType.REGULAR((8,)),
        ],
        compiler_params=pltpu.CompilerParams(
            collective_id=0, has_side_effects=True, vmem_limit_bytes=60 * 2**20
        ),
        name="filter_steps",
    )(
        observed,
        latent_noise,
        w_hidden,
        w_latent,
        w_frame,
        gate_bias.reshape(1, -1),
        w_prior,
        w_emit,
        w_emit_hidden,
        block_source,
        inner_offset,
        resample_flags,
    )
    return hidden, bound.reshape(1)


def solution(mesh):
    in_specs = (
        P("seq", None),
        P(None, None, ("seq", "dom")),
        P(),
        P(),
        P(),
        P(),
        P(),
        P(),
        P(),
        P("seq", None),
        P("seq", None),
        P(),
    )
    out_specs = (P(None, ("seq", "dom")), P("seq"))
    return jax.shard_map(body, mesh=mesh, in_specs=in_specs, out_specs=out_specs, check_vma=False)
```

```python
import functools
import math

import jax
import jax.numpy as jnp
from jax import lax
from jax.experimental import pallas as pl
from jax.experimental.pallas import tpu as pltpu
from jax.sharding import PartitionSpec as P

BLK = 128
F32 = jnp.float32
BF16 = jnp.bfloat16
MESH = pl.DeviceIdType.MESH
CH = 4


def mm(a, b):
    return jnp.dot(a, b, preferred_element_type=F32)


def sig(x):
    return 0.5 * jnp.tanh(0.5 * x) + 0.5


def cell_update(gates, old, n):
    in_gate = sig(gates[:n])
    forget = sig(gates[n : 2 * n])
    cand = jnp.tanh(gates[2 * n : 3 * n])
    out_gate = sig(gates[3 * n :])
    fresh = forget * old.astype(F32) + in_gate * cand
    return (out_gate * jnp.tanh(fresh)).astype(BF16), fresh.astype(BF16)


def split3(x):
    hi = x.astype(BF16)
    rest = x - hi.astype(F32)
    mid = rest.astype(BF16)
    return hi, mid, (rest - mid.astype(F32)).astype(BF16)


def kernel(
    D,
    obs_h,
    nz_h,
    wh_h,
    wl_h,
    wf_h,
    bias_h,
    wp_h,
    we_h,
    weh_h,
    bs_h,
    off_h,
    fl_h,
    h4,
    lse_all,
    used_o,
    wh,
    wlf,
    wf,
    tpose,
    bias,
    wp,
    we,
    weh,
    obs,
    obs_pad,
    nz,
    off,
    bs,
    fl,
    from_l,
    from_r,
    x0,
    x0_l,
    x0_r,
    x1,
    x1_l,
    x1_r,
    g1,
    ga,
    gb,
    hz,
    cz,
    h1,
    c1,
    hc,
    cc,
    h2,
    c2,
    h3,
    c3,
    lse_row,
    wsem,
    lsem,
    ssem,
    rsem,
    as_sem,
    ar_sem,
    near_sem,
):
    H = wh.shape[2]
    Z = we.shape[1]
    X = we.shape[0]
    HC = H // CH
    me = lax.axis_index("dom")
    right = lax.rem(me + 1, D)
    left = lax.rem(me + D - 1, D)
    has_r, has_l = me < D - 1, me > 0

    def signal(sem, dev, there):
        @pl.when(there)
        def _():
            pl.semaphore_signal(sem, inc=1, device_id={"dom": dev}, device_id_type=MESH)

    def partners(dist):
        return (
            (lax.rem(me + dist, D), me + dist < D),
            (lax.rem(me + D - dist, D), me >= dist),
        )

    def count(dist):
        return sum(jnp.where(there, 1, 0) for _, there in partners(dist))

    barrier = pltpu.get_barrier_semaphore()
    for dev, there in partners(1):
        signal(barrier, dev, there)

    def near_signal(i):
        for dev, there in partners(2**i):
            signal(near_sem.at[i], dev, there)

    def near_wait(i):
        pl.semaphore_wait(near_sem.at[i], count(2**i))

    small = []

    def fetch(src, dst):
        cp = pltpu.make_async_copy(src, dst, lsem.at[len(small)])
        cp.start()
        small.append(cp)
        return cp

    cp_wf = fetch(wf_h, wf)
    cp_bias = fetch(bias_h, bias)
    cp_obs = fetch(obs_h, obs)
    cp_off = fetch(off_h, off)
    cp_bs = fetch(bs_h, bs)
    cp_fl = fetch(fl_h, fl)

    def weight_copies(c):
        res = []
        for g in range(4):
            rows = pl.ds(g * H + c * HC, HC)
            res.append(
                pltpu.make_async_copy(
                    wh_h.at[rows, :], wh.at[c, pl.ds(g * HC, HC), :], wsem.at[0, c, g]
                )
            )
            res.append(
                pltpu.make_async_copy(
                    wl_h.at[rows, :], wlf.at[c, pl.ds(g * HC, HC), pl.ds(0, Z)], wsem.at[1, c, g]
                )
            )
        return res

    wcp = [weight_copies(c) for c in range(CH)]
    for c in range(CH):
        for cp in wcp[c]:
            cp.start(priority=1)
    cp_wp = fetch(wp_h, wp)
    cp_nz = fetch(nz_h, nz)
    cp_we = fetch(we_h, we)
    cp_weh = fetch(weh_h, weh)

    def link(side, k, src, dsts):
        return pltpu.make_async_remote_copy(
            src_ref=src,
            dst_ref=dsts[side],
            send_sem=ssem.at[side, k],
            recv_sem=rsem.at[side, k],
            device_id={"dom": (right, left)[side]},
            device_id_type=MESH,
        )

    sent = {}

    def send(k, src, *dsts):
        sent[k] = (src, dsts)
        for side, there in enumerate((has_r, has_l)):

            @pl.when(there)
            def _():
                link(side, k, src, dsts).start()

    def arrived(k):
        for side, there in enumerate((has_l, has_r)):

            @pl.when(there)
            def _():
                link(side, k, *sent[k]).wait_recv()

    def all_sent():
        for side, there in enumerate((has_r, has_l)):

            @pl.when(there)
            def _():
                for k in sent:
                    link(side, k, *sent[k]).wait_send()

    pl.semaphore_wait(barrier, count(1))
    send(0, nz_h.at[0], from_l.at[0], from_r.at[0])
    send(1, nz_h.at[1], from_l.at[1], from_r.at[1])
    near_signal(0)

    hz[...] = jnp.zeros_like(hz)
    cz[...] = jnp.zeros_like(cz)
    obs_pad[...] = jnp.zeros_like(obs_pad)
    tpose[X // 16 * 16 :, :] = jnp.zeros((BLK - X // 16 * 16, tpose.shape[1]), BF16)

    cp_bs.wait()
    cp_fl.wait()
    cp_off.wait()
    cp_obs.wait()
    f0, f1, f2 = fl[0] == 1, fl[1] == 1, fl[2] == 1

    around = range(-2, 3)
    place = [lax.rem(me + d + D, D) for d in around]

    def src(t, k, f):
        found = bs[t, place[2]]
        for d, p in zip(around, place):
            found = jnp.where(k - me == d, bs[t, p], found)
        return jnp.where(f, found, k)

    lane = lax.broadcasted_iota(jnp.int32, (1, BLK), 1).astype(F32)
    sub_i = lax.broadcasted_iota(jnp.int32, (BLK, BLK), 0)
    sub = sub_i.astype(F32)

    def flag_mask(f, shape):
        return jnp.broadcast_to(f.astype(jnp.int32), shape) > 0

    def offs(t, k, f):
        away = jnp.broadcast_to(k - me, (1, BLK))
        row = lane
        for d, p in zip(around, place):
            there = off[pl.ds(t, 1), pl.ds(pl.multiple_of(p * BLK, BLK), BLK)].astype(F32)
            row = jnp.where(jnp.logical_and(flag_mask(f, (1, BLK)), away == d), there, row)
        return row

    def onehot(row):
        return jnp.where(sub == row, 1.0, 0.0).astype(BF16)

    def comp(row, hot):
        return mm(jnp.broadcast_to(row, (16, BLK)).astype(BF16), hot)[:1]

    k2 = src(2, me, f2)
    k1 = src(1, k2, f1)
    s1 = src(1, me, f1)
    s0 = src(0, me, f0)
    both = jnp.logical_and(f0, f1)
    hot_q = onehot(offs(2, me, f2))
    hot_r = onehot(comp(offs(1, k2, f1), hot_q))
    hot_s = onehot(comp(offs(0, k1, f0), hot_r))
    hot_o1 = onehot(offs(1, me, f1))
    hot_o0 = onehot(comp(offs(0, s1, f0), hot_o1))
    hot_c0 = onehot(offs(0, me, f0))
    x0_src = jnp.where(f0, s0, s1)
    hop_o = jnp.where(both, s1, me)
    hop_l = jnp.where(f2, k2, hop_o)

    def pick(a, b, c, k):
        d = jnp.broadcast_to(k - me, a.shape)
        return jnp.where(d < 0, a, jnp.where(d > 0, c, b))

    def gather3(x, hot):
        hi, mid, lo = split3(x)
        out = mm(jnp.concatenate([hi, mid, lo], axis=0), hot)
        return out[:BLK] + out[BLK : 2 * BLK] + out[2 * BLK :]

    steps = obs.shape[0] - 1
    obs_pad[0 : steps + 1, 0:X] = obs[...].astype(F32)
    obs_t = jnp.transpose(obs_pad[...])

    def frame_col(t):
        return jnp.broadcast_to(obs_t[:, t : t + 1], (BLK, BLK))

    ones = jnp.logical_and(sub_i >= 96, sub_i < 99)
    tails = [jnp.where(ones, 1.0, frame_col(t)).astype(BF16) for t in range(steps)]

    cp_wf.wait()
    cp_bias.wait()
    tpose[0:X, :] = wf[...]
    hi, mid, lo = (p.astype(F32) for p in split3(bias[...]))
    r16 = lax.broadcasted_iota(jnp.int32, (16, bias.shape[1]), 0)
    tpose[96:112, :] = jnp.where(
        r16 == 0, hi, jnp.where(r16 == 1, mid, jnp.where(r16 == 2, lo, 0.0))
    ).astype(BF16)
    for c in range(CH):
        for g in range(4):
            for i in range(0, HC, BLK):
                rows = g * H + c * HC + i
                wlf[c, g * HC + i : g * HC + i + BLK, Z : Z + BLK] = jnp.transpose(
                    tpose[:, rows : rows + BLK]
                )

    def run_layer(gates, elem):
        bufs = (ga, gb)
        for c in range(CH):
            val = gates(c)
            bufs[c % 2][:, : val.shape[1]] = val
            if c:
                elem(c - 1, bufs[(c - 1) % 2])
        elem(CH - 1, bufs[(CH - 1) % 2])

    def elem_of(n, old, h_out, c_out):
        def elem(c, buf):
            rows = slice(c * HC, (c + 1) * HC)
            h, s = cell_update(buf[:, :n], old[rows, :n], HC)
            h_out[rows, :n] = h
            if c_out is not None:
                c_out[rows, :n] = s

        return elem

    def moments(h):
        p = mm(wp[...], h)
        return p[:Z], jnp.exp(0.5 * jnp.tanh(p[Z:]))

    def increment(t, lat, h):
        pred = mm(we[...], lat) + mm(weh[...], h)
        target = frame_col(t + 1)[:X]
        return jnp.sum(pred * (target - 0.5 * pred), axis=0, keepdims=True)

    lat_tail0 = jnp.concatenate([jnp.zeros((Z, BLK), BF16), tails[0]], axis=0)

    for c in range(CH):
        for cp in wcp[c]:
            cp.wait()
    cp_wp.wait()
    cp_nz.wait()
    cp_we.wait()
    cp_weh.wait()
    near_wait(0)
    near_signal(1)
    run_layer(lambda c: mm(wh[c], hz[...]) + mm(wlf[c], lat_tail0), elem_of(BLK, cz, h1, c1))
    mean0, std0 = moments(h1[...])

    arrived(0)
    n0 = pick(from_l[0], nz[0], from_r[0], x0_src)
    x0[...] = (mean0 + std0 * n0).astype(BF16)
    arrived(1)
    x1[...] = pick(from_l[1], nz[1], from_r[1], s1)
    near_wait(1)
    send(2, x0, x0_l, x0_r)
    send(3, x1, x1_l, x1_r)
    send(4, nz_h.at[2], from_l.at[2], from_r.at[2])
    near_signal(2)
    lw0 = increment(0, (mean0 + std0 * nz[0]).astype(BF16), h1[...])

    for c in range(CH):
        g1[c] = mm(wh[c], h1[...])

    lat_c = mm(
        (mean0 + std0 * pick(from_l[0], nz[0], from_r[0], s0)).astype(BF16), hot_c0
    ).astype(BF16)
    tail_c = jnp.concatenate([lat_c, tails[1]], axis=0)
    run_layer(lambda c: g1[c] + mm(wlf[c], tail_c), elem_of(BLK, c1, hc, None))
    mean_c, std_c = moments(hc[...])
    inc_c = increment(1, (mean_c + std_c * nz[1]).astype(BF16), hc[...])
    lw1 = jnp.where(flag_mask(f0, (1, BLK)), 0.0, lw0) + inc_c

    near_wait(2)
    near_signal(3)
    arrived(2)
    x0s = (x0_l[...].astype(F32), x0[...].astype(F32), x0_r[...].astype(F32))
    lat_o = mm(pick(*x0s, hop_o).astype(BF16), hot_o0).astype(BF16)
    lat_l = mm(pick(*x0s, hop_l).astype(BF16), hot_s).astype(BF16)
    tail_ol = jnp.concatenate(
        [
            jnp.concatenate([lat_o, lat_l], axis=1),
            jnp.concatenate([tails[1], tails[1]], axis=1),
        ],
        axis=0,
    )

    def gates1(c):
        g = g1[c]
        return jnp.concatenate([g, g], axis=1) + mm(wlf[c], tail_ol)

    def elem1(c, buf):
        rows = slice(c * HC, (c + 1) * HC)
        old = c1[rows, :]
        h, s = cell_update(buf[...], jnp.concatenate([old, old], axis=1), HC)
        h2[rows, :] = h
        c2[rows, :] = s

    run_layer(gates1, elem1)
    m1, sd1 = moments(h2[...])
    arrived(3)
    n1_o = gather3(x1[...], hot_o1)
    n1_l = gather3(pick(x1_l[...], x1[...], x1_r[...], k2), hot_r)
    lat1 = (m1 + sd1 * jnp.concatenate([n1_o, n1_l], axis=1)).astype(BF16)

    tail2 = jnp.concatenate(
        [lat1, jnp.concatenate([tails[2], tails[2]], axis=1)], axis=0
    )
    run_layer(
        lambda c: mm(wh[c], h2[...]) + mm(wlf[c], tail2), elem_of(2 * BLK, c2, h3, c3)
    )
    near_wait(3)
    near_signal(4)
    m2, sd2 = moments(h3[...])
    arrived(4)
    n2_l = gather3(pick(from_l[2], nz[2], from_r[2], k2), hot_q)
    lat2 = (m2 + sd2 * jnp.concatenate([nz[2], n2_l], axis=1)).astype(BF16)
    inc2 = increment(2, lat2[:, :BLK], h3[:, :BLK])
    lw2 = jnp.where(flag_mask(f1, (1, BLK)), 0.0, lw1) + inc2

    tail3 = jnp.concatenate([lat2[:, BLK:], tails[3]], axis=0)

    def gates3(c):
        return mm(wh[c], h3[:, BLK:]) + mm(wlf[c], tail3)

    def elem3(c, buf):
        rows = slice(c * HC, (c + 1) * HC)
        h, _ = cell_update(buf[:, :BLK], c3[rows, BLK:], HC)
        h4[rows, :] = h

    run_layer(gates3, elem3)
    m3, sd3 = moments(h4[...])
    lat3 = (m3 + sd3 * nz[3]).astype(BF16)
    lw3 = jnp.where(flag_mask(f2, (1, BLK)), 0.0, lw2) + increment(3, lat3, h4[...])

    def lse(lw):
        peak = jnp.max(lw, axis=1, keepdims=True)
        return peak + jnp.log(jnp.sum(jnp.exp(lw - peak), axis=1, keepdims=True))

    lane_i = lax.broadcasted_iota(jnp.int32, (1, BLK), 1)
    row = jnp.zeros((1, BLK), F32)
    for t, lw in enumerate((lw0, lw1, lw2, lw3)):
        row = jnp.where(lane_i == t, lse(lw), row)
    lse_row[...] = row
    lse_all[pl.ds(me, 1)] = row[None]
    used = lane_i == steps - 1
    for t, f in enumerate((f0, f1, f2)):
        used = jnp.logical_or(used, jnp.logical_and(lane_i == t, flag_mask(f, (1, BLK))))
    used_o[...] = jnp.where(used, 1.0, 0.0)
    near_wait(4)
    pushes = []
    for d in range(1, D):
        dev = lax.rem(me + d, D)
        cp = pltpu.make_async_remote_copy(
            src_ref=lse_row,
            dst_ref=lse_all.at[me],
            send_sem=as_sem.at[d],
            recv_sem=ar_sem.at[me],
            device_id={"dom": dev},
            device_id_type=MESH,
        )
        cp.start()
        pushes.append(cp)
    all_sent()
    for d in range(1, D):
        frm = lax.rem(me + d, D)
        pltpu.make_async_remote_copy(
            src_ref=lse_row,
            dst_ref=lse_all.at[frm],
            send_sem=as_sem.at[d],
            recv_sem=ar_sem.at[frm],
            device_id={"dom": frm},
            device_id_type=MESH,
        ).wait_recv()
    for cp in pushes:
        cp.wait_send()


def finish(h_ref, lse_all, used, hid_o, bnd_o, sem):
    out_cp = pltpu.make_async_copy(h_ref, hid_o, sem)
    out_cp.start()
    every = lse_all[...]
    peak = jnp.max(every, axis=0)
    total = jnp.log(jnp.sum(jnp.exp(every - peak[None]), axis=0))
    level = peak + total - math.log(every.shape[0] * BLK)
    bnd_o[...] = jnp.sum(jnp.where(used[...] > 0, level, 0.0), axis=1, keepdims=True)
    out_cp.wait()


def body(
    observed,
    latent_noise,
    w_hidden,
    w_latent,
    w_frame,
    gate_bias,
    w_prior,
    w_emit,
    w_emit_hidden,
    block_source,
    inner_offset,
    resample_flags,
):
    D = lax.axis_size("dom")
    steps, Z, n = latent_noise.shape
    H = w_hidden.shape[1]
    X = w_emit.shape[0]
    G = 4 * H // CH
    V = pltpu.VMEM
    DMA = pltpu.SemaphoreType.DMA
    pinned = [
        pltpu.with_memory_space_constraint(x, pltpu.HBM)
        for x in (
            observed,
            latent_noise,
            w_hidden,
            w_latent,
            w_frame,
            gate_bias.reshape(1, -1),
            w_prior,
            w_emit,
            w_emit_hidden,
            block_source,
            inner_offset,
            resample_flags,
        )
    ]
    last_hidden, lse_all, used = pl.pallas_call(
        functools.partial(kernel, D),
        out_shape=(
            jax.ShapeDtypeStruct((H, n), BF16),
            jax.ShapeDtypeStruct((D, 1, BLK), F32),
            jax.ShapeDtypeStruct((1, BLK), F32),
        ),
        in_specs=[pl.BlockSpec(memory_space=pltpu.HBM)] * 12,
        out_specs=(pl.BlockSpec(memory_space=pltpu.VMEM),) * 3,
        scratch_shapes=[
            V((CH, G, H), BF16),
            V((CH, G, Z + BLK), BF16),
            V((X, 4 * H), BF16),
            V((BLK, 4 * H), BF16),
            V((1, 4 * H), F32),
            V((2 * Z, H), BF16),
            V((X, Z), BF16),
            V((X, H), BF16),
            V((steps + 1, X), BF16),
            V((BLK, BLK), F32),
            V((steps, Z, n), F32),
            V(inner_offset.shape, jnp.int32),
            pltpu.SMEM(block_source.shape, jnp.int32),
            pltpu.SMEM(resample_flags.shape, jnp.int32),
            V((3, Z, n), F32),
            V((3, Z, n), F32),
            V((Z, n), BF16),
            V((Z, n), BF16),
            V((Z, n), BF16),
            V((Z, n), F32),
            V((Z, n), F32),
            V((Z, n), F32),
            V((CH, G, n), F32),
            V((G, 2 * n), F32),
            V((G, 2 * n), F32),
            V((H, n), BF16),
            V((H, n), BF16),
            V((H, n), BF16),
            V((H, n), BF16),
            V((H, n), BF16),
            V((H, n), BF16),
            V((H, 2 * n), BF16),
            V((H, 2 * n), BF16),
            V((H, 2 * n), BF16),
            V((H, 2 * n), BF16),
            V((1, BLK), F32),
            DMA((2, CH, 4)),
            DMA((16,)),
            DMA((2, 5)),
            DMA((2, 5)),
            DMA((D,)),
            DMA((D,)),
            pltpu.SemaphoreType.REGULAR((8,)),
        ],
        compiler_params=pltpu.CompilerParams(
            collective_id=0, has_side_effects=True, vmem_limit_bytes=32 * 2**20
        ),
        name="filter_steps",
    )(*pinned)
    hidden, bound = pl.pallas_call(
        finish,
        out_shape=(
            jax.ShapeDtypeStruct((H, n), BF16),
            jax.ShapeDtypeStruct((1, 1), F32),
        ),
        in_specs=[pl.BlockSpec(memory_space=pltpu.VMEM)] * 3,
        out_specs=(
            pl.BlockSpec(memory_space=pl.ANY),
            pl.BlockSpec(memory_space=pltpu.VMEM),
        ),
        scratch_shapes=[DMA],
        compiler_params=pltpu.CompilerParams(vmem_limit_bytes=2 * 2**20),
        name="finish",
    )(last_hidden, lse_all, used)
    return hidden, bound.reshape(1)


def solution(mesh):
    in_specs = (
        P("seq", None),
        P(None, None, ("seq", "dom")),
        P(),
        P(),
        P(),
        P(),
        P(),
        P(),
        P(),
        P("seq", None),
        P("seq", None),
        P(),
    )
    out_specs = (P(None, ("seq", "dom")), P("seq"))
    return jax.shard_map(body, mesh=mesh, in_specs=in_specs, out_specs=out_specs, check_vma=False)
```

```python
import functools
import math

import jax
import jax.numpy as jnp
from jax import lax
from jax.experimental import pallas as pl
from jax.experimental.pallas import tpu as pltpu
from jax.sharding import PartitionSpec as P

BLK = 128
F32 = jnp.float32
BF16 = jnp.bfloat16
MESH = pl.DeviceIdType.MESH
CH = 4


def mm(a, b):
    return jnp.dot(a, b, preferred_element_type=F32)


def sig(x):
    return 0.5 * jnp.tanh(0.5 * x) + 0.5


def cell_update(gates, old, n):
    in_gate = sig(gates[:n])
    forget = sig(gates[n : 2 * n])
    cand = jnp.tanh(gates[2 * n : 3 * n])
    out_gate = sig(gates[3 * n :])
    fresh = forget * old.astype(F32) + in_gate * cand
    return (out_gate * jnp.tanh(fresh)).astype(BF16), fresh.astype(BF16)


def split3(x):
    hi = x.astype(BF16)
    rest = x - hi.astype(F32)
    mid = rest.astype(BF16)
    return hi, mid, (rest - mid.astype(F32)).astype(BF16)


def kernel(
    D,
    obs_h,
    nz_h,
    wh_h,
    wl_h,
    wf_h,
    bias_h,
    wp_h,
    we_h,
    weh_h,
    bs_h,
    off_h,
    fl_h,
    h4,
    lse_all,
    used_o,
    wh,
    wlf,
    wf,
    tpose,
    bias,
    wp,
    we,
    weh,
    obs,
    obs_pad,
    nz,
    off,
    bs,
    fl,
    from_l,
    from_r,
    x0,
    x0_l,
    x0_r,
    x1,
    x1_l,
    x1_r,
    g1,
    ga,
    gb,
    gc,
    gd,
    hz,
    cz,
    h1,
    c1,
    hc,
    h2,
    c2,
    h3,
    c3,
    lse_row,
    wsem,
    lsem,
    ssem,
    rsem,
    as_sem,
    ar_sem,
    near_sem,
):
    H = wh.shape[3]
    Z = we.shape[1]
    X = we.shape[0]
    HC = H // CH
    me = lax.axis_index("dom")
    right = lax.rem(me + 1, D)
    left = lax.rem(me + D - 1, D)
    has_r, has_l = me < D - 1, me > 0

    def signal(sem, dev, there):
        @pl.when(there)
        def _():
            pl.semaphore_signal(sem, inc=1, device_id={"dom": dev}, device_id_type=MESH)

    def partners(dist):
        return (
            (lax.rem(me + dist, D), me + dist < D),
            (lax.rem(me + D - dist, D), me >= dist),
        )

    def count(dist):
        return sum(jnp.where(there, 1, 0) for _, there in partners(dist))

    barrier = pltpu.get_barrier_semaphore()
    for dev, there in partners(1):
        signal(barrier, dev, there)

    def near_signal(i):
        for dev, there in partners(2**i):
            signal(near_sem.at[i], dev, there)

    def near_wait(i):
        pl.semaphore_wait(near_sem.at[i], count(2**i))

    small = []

    def fetch(src, dst):
        cp = pltpu.make_async_copy(src, dst, lsem.at[len(small)])
        cp.start()
        small.append(cp)
        return cp

    cp_n01 = fetch(nz_h.at[pl.ds(0, 2)], nz.at[pl.ds(0, 2)])
    cp_wf = fetch(wf_h, wf)
    cp_bias = fetch(bias_h, bias)
    cp_obs = fetch(obs_h, obs)
    cp_off = fetch(off_h, off)
    cp_bs = fetch(bs_h, bs)
    cp_fl = fetch(fl_h, fl)

    wcp = [
        (
            pltpu.make_async_copy(wh_h.at[:, c], wh.at[c], wsem.at[0, c]),
            pltpu.make_async_copy(wl_h.at[:, c], wlf.at[c, :, :, pl.ds(0, Z)], wsem.at[1, c]),
        )
        for c in range(CH)
    ]
    for pair in wcp:
        for cp in pair:
            cp.start(priority=1)
    cp_wp = fetch(wp_h, wp)
    cp_n23 = fetch(nz_h.at[pl.ds(2, 2)], nz.at[pl.ds(2, 2)])
    cp_we = fetch(we_h, we)
    cp_weh = fetch(weh_h, weh)

    def link(side, k, src, dsts):
        return pltpu.make_async_remote_copy(
            src_ref=src,
            dst_ref=dsts[side],
            send_sem=ssem.at[side, max(k - 2, 0)],
            recv_sem=rsem.at[side, k],
            device_id={"dom": (right, left)[side]},
            device_id_type=MESH,
        )

    sent = {}

    def send(k, src, *dsts):
        sent[k] = (src, dsts)
        for side, there in enumerate((has_r, has_l)):

            @pl.when(there)
            def _():
                link(side, k, src, dsts).start()

    def arrived(k):
        for side, there in enumerate((has_l, has_r)):

            @pl.when(there)
            def _():
                link(side, k, *sent[k]).wait_recv()

    def all_sent():
        for side, there in enumerate((has_r, has_l)):

            @pl.when(there)
            def _():
                noise = pl.ds(0, 3)
                link(side, 0, nz_h.at[noise], (from_l.at[noise], from_r.at[noise])).wait_send()
                for k in (3, 4):
                    link(side, k, *sent[k]).wait_send()

    pl.semaphore_wait(barrier, count(1))
    cp_n01.wait()
    for t in range(2):
        send(t, nz.at[t], from_l.at[t], from_r.at[t])
    send(2, nz_h.at[2], from_l.at[2], from_r.at[2])
    near_signal(0)

    hz[...] = jnp.zeros_like(hz)
    cz[...] = jnp.zeros_like(cz)
    obs_pad[...] = jnp.zeros_like(obs_pad)
    tpose[X // 16 * 16 :, :] = jnp.zeros((BLK - X // 16 * 16, tpose.shape[1]), BF16)

    cp_bs.wait()
    cp_fl.wait()
    cp_off.wait()
    cp_obs.wait()
    f0, f1, f2 = fl[0] == 1, fl[1] == 1, fl[2] == 1

    around = range(-2, 3)
    place = [lax.rem(me + d + D, D) for d in around]

    def src(t, k, f):
        found = bs[t, place[2]]
        for d, p in zip(around, place):
            found = jnp.where(k - me == d, bs[t, p], found)
        return jnp.where(f, found, k)

    lane = lax.broadcasted_iota(jnp.int32, (1, BLK), 1).astype(F32)
    sub_i = lax.broadcasted_iota(jnp.int32, (BLK, BLK), 0)
    sub = sub_i.astype(F32)

    def flag_mask(f, shape):
        return jnp.broadcast_to(f.astype(jnp.int32), shape) > 0

    def offs(t, k, f):
        away = jnp.broadcast_to(k - me, (1, BLK))
        row = lane
        for d, p in zip(around, place):
            there = off[pl.ds(t, 1), pl.ds(pl.multiple_of(p * BLK, BLK), BLK)].astype(F32)
            row = jnp.where(jnp.logical_and(flag_mask(f, (1, BLK)), away == d), there, row)
        return row

    def onehot(row):
        return jnp.where(sub == row, 1.0, 0.0).astype(BF16)

    def comp(row, hot):
        return mm(jnp.broadcast_to(row, (16, BLK)).astype(BF16), hot)[:1]

    k2 = src(2, me, f2)
    k1 = src(1, k2, f1)
    s1 = src(1, me, f1)
    s0 = src(0, me, f0)
    both = jnp.logical_and(f0, f1)
    hot_q = onehot(offs(2, me, f2))
    hot_r = onehot(comp(offs(1, k2, f1), hot_q))
    hot_s = onehot(comp(offs(0, k1, f0), hot_r))
    hot_o1 = onehot(offs(1, me, f1))
    hot_o0 = onehot(comp(offs(0, s1, f0), hot_o1))
    hot_c0 = onehot(offs(0, me, f0))
    x0_src = jnp.where(f0, s0, s1)
    hop_o = jnp.where(both, s1, me)
    hop_l = jnp.where(f2, k2, hop_o)

    def pick(a, b, c, k):
        d = jnp.broadcast_to(k - me, a.shape)
        return jnp.where(d < 0, a, jnp.where(d > 0, c, b))

    def gather3(x, hot):
        hi, mid, lo = split3(x)
        out = mm(jnp.concatenate([hi, mid, lo], axis=0), hot)
        return out[:BLK] + out[BLK : 2 * BLK] + out[2 * BLK :]

    steps = obs.shape[0] - 1
    obs_pad[0 : steps + 1, 0:X] = obs[...].astype(F32)
    obs_t = jnp.transpose(obs_pad[...])

    def frame_col(t):
        return jnp.broadcast_to(obs_t[:, t : t + 1], (BLK, BLK))

    ones = jnp.logical_and(sub_i >= 96, sub_i < 99)
    tails = [jnp.where(ones, 1.0, frame_col(t)).astype(BF16) for t in range(steps)]

    cp_wf.wait()
    cp_bias.wait()
    tpose[0:X, :] = wf[...]
    hi, mid, lo = (p.astype(F32) for p in split3(bias[...]))
    r16 = lax.broadcasted_iota(jnp.int32, (16, bias.shape[1]), 0)
    tpose[96:112, :] = jnp.where(
        r16 == 0, hi, jnp.where(r16 == 1, mid, jnp.where(r16 == 2, lo, 0.0))
    ).astype(BF16)
    for c in range(CH):
        for g in range(4):
            for i in range(0, HC, BLK):
                rows = g * H + c * HC + i
                wlf[c, g, i : i + BLK, Z : Z + BLK] = jnp.transpose(
                    tpose[:, rows : rows + BLK]
                )

    def run_layer(gates, elem):
        bufs = (ga, gb)
        for c in range(CH):
            val = gates(c)
            bufs[c % 2][:, : val.shape[1]] = val
            if c:
                elem(c - 1, bufs[(c - 1) % 2])
        elem(CH - 1, bufs[(CH - 1) % 2])

    def elem_of(n, old, h_out, c_out):
        def elem(c, buf):
            rows = slice(c * HC, (c + 1) * HC)
            h, s = cell_update(buf[:, :n], old[rows, :n], HC)
            h_out[rows, :n] = h
            if c_out is not None:
                c_out[rows, :n] = s

        return elem

    def moments(h):
        p = mm(wp[...], h)
        return p[:Z], jnp.exp(0.5 * jnp.tanh(p[Z:]))

    def increment(t, lat, h):
        pred = mm(we[...], lat) + mm(weh[...], h)
        target = frame_col(t + 1)[:X]
        return jnp.sum(pred * (target - 0.5 * pred), axis=0, keepdims=True)

    lat_tail0 = jnp.concatenate([jnp.zeros((Z, BLK), BF16), tails[0]], axis=0)

    def w_h(c):
        return wh[c].reshape(4 * HC, H)

    def w_lf(c):
        return wlf[c].reshape(4 * HC, Z + BLK)

    def gates0(c):
        if c % (CH // 2) == 0:
            for pair in wcp[c : c + CH // 2]:
                for cp in pair:
                    cp.wait()
        return mm(w_h(c), hz[...]) + mm(w_lf(c), lat_tail0)

    run_layer(gates0, elem_of(BLK, cz, h1, c1))
    cp_wp.wait()
    cp_n23.wait()
    cp_we.wait()
    cp_weh.wait()
    mean0, std0 = moments(h1[...])

    arrived(0)
    n0 = pick(from_l[0], nz[0], from_r[0], x0_src)
    x0[...] = (mean0 + std0 * n0).astype(BF16)
    near_wait(0)
    send(3, x0, x0_l, x0_r)
    arrived(1)
    x1[...] = pick(from_l[1], nz[1], from_r[1], s1)
    near_signal(1)
    send(4, x1, x1_l, x1_r)
    lw0 = increment(0, (mean0 + std0 * nz[0]).astype(BF16), h1[...])

    lat_c = mm(
        (mean0 + std0 * pick(from_l[0], nz[0], from_r[0], s0)).astype(BF16), hot_c0
    ).astype(BF16)
    tail_c = jnp.concatenate([lat_c, tails[1]], axis=0)

    def gates_c(c):
        g = mm(w_h(c), h1[...])
        g1[c] = g
        return g + mm(w_lf(c), tail_c)

    run_layer(gates_c, elem_of(BLK, c1, hc, None))
    near_wait(1)
    arrived(3)
    near_signal(2)
    mean_c, std_c = moments(hc[...])
    inc_c = increment(1, (mean_c + std_c * nz[1]).astype(BF16), hc[...])
    lw1 = jnp.where(flag_mask(f0, (1, BLK)), 0.0, lw0) + inc_c

    x0s = (x0_l[...].astype(F32), x0[...].astype(F32), x0_r[...].astype(F32))
    lat_o = mm(pick(*x0s, hop_o).astype(BF16), hot_o0).astype(BF16)
    lat_l = mm(pick(*x0s, hop_l).astype(BF16), hot_s).astype(BF16)
    tail_ol = jnp.concatenate(
        [
            jnp.concatenate([lat_o, lat_l], axis=1),
            jnp.concatenate([tails[1], tails[1]], axis=1),
        ],
        axis=0,
    )

    def gates1(c):
        g = g1[c]
        return jnp.concatenate([g, g], axis=1) + mm(w_lf(c), tail_ol)

    def elem1(c, buf):
        rows = slice(c * HC, (c + 1) * HC)
        old = c1[rows, :]
        h, s = cell_update(buf[...], jnp.concatenate([old, old], axis=1), HC)
        h2[rows, :] = h
        c2[rows, :] = s

    run_layer(gates1, elem1)
    m1, sd1 = moments(h2[...])
    early = (gc, gd)
    for c in range(2):
        early[c][...] = mm(w_h(c), h2[...])
    near_wait(2)
    arrived(4)
    arrived(2)
    near_signal(3)
    n1_o = gather3(x1[...], hot_o1)
    n1_l = gather3(pick(x1_l[...], x1[...], x1_r[...], k2), hot_r)
    lat1 = (m1 + sd1 * jnp.concatenate([n1_o, n1_l], axis=1)).astype(BF16)

    tail2 = jnp.concatenate(
        [lat1, jnp.concatenate([tails[2], tails[2]], axis=1)], axis=0
    )

    def gates2(c):
        part = early[c][...] if c < 2 else mm(w_h(c), h2[...])
        return part + mm(w_lf(c), tail2)

    run_layer(gates2, elem_of(2 * BLK, c2, h3, c3))
    near_wait(3)
    near_signal(4)
    m2, sd2 = moments(h3[...])
    n2_l = gather3(pick(from_l[2], nz[2], from_r[2], k2), hot_q)
    lat2 = (m2 + sd2 * jnp.concatenate([nz[2], n2_l], axis=1)).astype(BF16)
    inc2 = increment(2, lat2[:, :BLK], h3[:, :BLK])
    lw2 = jnp.where(flag_mask(f1, (1, BLK)), 0.0, lw1) + inc2

    tail3 = jnp.concatenate([lat2[:, BLK:], tails[3]], axis=0)

    def gates3(c):
        return mm(w_h(c), h3[:, BLK:]) + mm(w_lf(c), tail3)

    def elem3(c, buf):
        rows = slice(c * HC, (c + 1) * HC)
        h, _ = cell_update(buf[:, :BLK], c3[rows, BLK:], HC)
        h4[rows, :] = h

    run_layer(gates3, elem3)
    m3, sd3 = moments(h4[...])
    lat3 = (m3 + sd3 * nz[3]).astype(BF16)
    lw3 = jnp.where(flag_mask(f2, (1, BLK)), 0.0, lw2) + increment(3, lat3, h4[...])

    def lse(lw):
        peak = jnp.max(lw, axis=1, keepdims=True)
        return peak + jnp.log(jnp.sum(jnp.exp(lw - peak), axis=1, keepdims=True))

    lane_i = lax.broadcasted_iota(jnp.int32, (1, BLK), 1)
    row = jnp.zeros((1, BLK), F32)
    for t, lw in enumerate((lw0, lw1, lw2, lw3)):
        row = jnp.where(lane_i == t, lse(lw), row)
    lse_row[...] = row
    lse_all[pl.ds(me, 1)] = row[None]
    used = lane_i == steps - 1
    for t, f in enumerate((f0, f1, f2)):
        used = jnp.logical_or(used, jnp.logical_and(lane_i == t, flag_mask(f, (1, BLK))))
    used_o[...] = jnp.where(used, 1.0, 0.0)
    near_wait(4)
    for d in range(1, D):
        pltpu.make_async_remote_copy(
            src_ref=lse_row,
            dst_ref=lse_all.at[me],
            send_sem=as_sem,
            recv_sem=ar_sem,
            device_id={"dom": lax.rem(me + d, D)},
            device_id_type=MESH,
        ).start()
    all_sent()
    others = lse_all.at[pl.ds(0, D - 1)]
    every = pltpu.make_async_remote_copy(
        src_ref=others,
        dst_ref=others,
        send_sem=as_sem,
        recv_sem=ar_sem,
        device_id={"dom": right},
        device_id_type=MESH,
    )
    every.wait_recv()
    every.wait_send()


def finish(h_ref, lse_all, used, hid_o, bnd_o, sem):
    out_cp = pltpu.make_async_copy(h_ref, hid_o, sem)
    out_cp.start()
    every = lse_all[...]
    peak = jnp.max(every, axis=0)
    total = jnp.log(jnp.sum(jnp.exp(every - peak[None]), axis=0))
    level = peak + total - math.log(every.shape[0] * BLK)
    bnd_o[...] = jnp.sum(jnp.where(used[...] > 0, level, 0.0), axis=1, keepdims=True)
    out_cp.wait()


def body(
    observed,
    latent_noise,
    w_hidden,
    w_latent,
    w_frame,
    gate_bias,
    w_prior,
    w_emit,
    w_emit_hidden,
    block_source,
    inner_offset,
    resample_flags,
):
    D = lax.axis_size("dom")
    steps, Z, n = latent_noise.shape
    H = w_hidden.shape[1]
    X = w_emit.shape[0]
    G = 4 * H // CH
    V = pltpu.VMEM
    DMA = pltpu.SemaphoreType.DMA
    pinned = [
        pltpu.with_memory_space_constraint(x, pltpu.HBM)
        for x in (
            observed,
            latent_noise,
            w_hidden.reshape(4, CH, H // CH, H),
            w_latent.reshape(4, CH, H // CH, Z),
            w_frame,
            gate_bias.reshape(1, -1),
            w_prior,
            w_emit,
            w_emit_hidden,
            block_source,
            inner_offset,
            resample_flags,
        )
    ]
    last_hidden, lse_all, used = pl.pallas_call(
        functools.partial(kernel, D),
        out_shape=(
            jax.ShapeDtypeStruct((H, n), BF16),
            jax.ShapeDtypeStruct((D, 1, BLK), F32),
            jax.ShapeDtypeStruct((1, BLK), F32),
        ),
        in_specs=[pl.BlockSpec(memory_space=pltpu.HBM)] * 12,
        out_specs=(pl.BlockSpec(memory_space=pltpu.VMEM),) * 3,
        scratch_shapes=[
            V((CH, 4, H // CH, H), BF16),
            V((CH, 4, H // CH, Z + BLK), BF16),
            V((X, 4 * H), BF16),
            V((BLK, 4 * H), BF16),
            V((1, 4 * H), F32),
            V((2 * Z, H), BF16),
            V((X, Z), BF16),
            V((X, H), BF16),
            V((steps + 1, X), BF16),
            V((BLK, BLK), F32),
            V((steps, Z, n), F32),
            V(inner_offset.shape, jnp.int32),
            pltpu.SMEM(block_source.shape, jnp.int32),
            pltpu.SMEM(resample_flags.shape, jnp.int32),
            V((3, Z, n), F32),
            V((3, Z, n), F32),
            V((Z, n), BF16),
            V((Z, n), BF16),
            V((Z, n), BF16),
            V((Z, n), F32),
            V((Z, n), F32),
            V((Z, n), F32),
            V((CH, G, n), F32),
            V((G, 2 * n), F32),
            V((G, 2 * n), F32),
            V((G, 2 * n), F32),
            V((G, 2 * n), F32),
            V((H, n), BF16),
            V((H, n), BF16),
            V((H, n), BF16),
            V((H, n), BF16),
            V((H, n), BF16),
            V((H, 2 * n), BF16),
            V((H, 2 * n), BF16),
            V((H, 2 * n), BF16),
            V((H, 2 * n), BF16),
            V((1, BLK), F32),
            DMA((2, CH)),
            DMA((11,)),
            DMA((2, 3)),
            DMA((2, 5)),
            DMA,
            DMA,
            pltpu.SemaphoreType.REGULAR((5,)),
        ],
        compiler_params=pltpu.CompilerParams(
            collective_id=0, has_side_effects=True, vmem_limit_bytes=32 * 2**20
        ),
        name="filter_steps",
    )(*pinned)
    hidden, bound = pl.pallas_call(
        finish,
        out_shape=(
            jax.ShapeDtypeStruct((H, n), BF16),
            jax.ShapeDtypeStruct((1, 1), F32),
        ),
        in_specs=[pl.BlockSpec(memory_space=pltpu.VMEM)] * 3,
        out_specs=(
            pl.BlockSpec(memory_space=pl.ANY),
            pl.BlockSpec(memory_space=pltpu.VMEM),
        ),
        scratch_shapes=[DMA],
        compiler_params=pltpu.CompilerParams(vmem_limit_bytes=2 * 2**20),
        name="finish",
    )(last_hidden, lse_all, used)
    return hidden, bound.reshape(1)


def solution(mesh):
    in_specs = (
        P("seq", None),
        P(None, None, ("seq", "dom")),
        P(),
        P(),
        P(),
        P(),
        P(),
        P(),
        P(),
        P("seq", None),
        P("seq", None),
        P(),
    )
    out_specs = (P(None, ("seq", "dom")), P("seq"))
    return jax.shard_map(body, mesh=mesh, in_specs=in_specs, out_specs=out_specs, check_vma=False)
```

```python
import functools
import math

import jax
import jax.numpy as jnp
from jax import lax
from jax.experimental import pallas as pl
from jax.experimental.pallas import tpu as pltpu
from jax.sharding import PartitionSpec as P

BLK = 128
F32 = jnp.float32
BF16 = jnp.bfloat16
MESH = pl.DeviceIdType.MESH
CH = 8


def mm(a, b):
    return jnp.dot(a, b, preferred_element_type=F32)


def sig(x):
    return 0.5 * jnp.tanh(0.5 * x) + 0.5


def cell_update(gates, old, n):
    in_gate = sig(gates[:n])
    forget = sig(gates[n : 2 * n])
    cand = jnp.tanh(gates[2 * n : 3 * n])
    out_gate = sig(gates[3 * n :])
    fresh = forget * old.astype(F32) + in_gate * cand
    return (out_gate * jnp.tanh(fresh)).astype(BF16), fresh.astype(BF16)


def split3(x):
    hi = x.astype(BF16)
    rest = x - hi.astype(F32)
    mid = rest.astype(BF16)
    return hi, mid, (rest - mid.astype(F32)).astype(BF16)


def kernel(
    D,
    obs_h,
    nz_h,
    wh_h,
    wl_h,
    wf_h,
    bias_h,
    wp_h,
    we_h,
    weh_h,
    bs_h,
    off_h,
    fl_h,
    h4,
    lse_all,
    used_o,
    wh,
    wlf,
    wf,
    tpose,
    bias,
    wp,
    we,
    weh,
    obs,
    obs_pad,
    nz,
    off,
    bs,
    fl,
    rx,
    x0,
    x0_far,
    x1_far,
    g1,
    ga,
    gb,
    gc,
    hz,
    cz,
    h1,
    c1,
    hc,
    h2,
    c2,
    h3,
    c3,
    lse_row,
    wsem,
    lsem,
    ssem,
    rsem,
    as_sem,
    ar_sem,
    near_sem,
):
    H = wh.shape[3]
    Z = we.shape[1]
    X = we.shape[0]
    HC = H // CH
    me = lax.axis_index("dom")
    right = lax.rem(me + 1, D)
    left = lax.rem(me + D - 1, D)

    def signal(sem, dev, there):
        @pl.when(there)
        def _():
            pl.semaphore_signal(sem, inc=1, device_id={"dom": dev}, device_id_type=MESH)

    def partners(dist):
        return (
            (lax.rem(me + dist, D), me + dist < D),
            (lax.rem(me + D - dist, D), me >= dist),
        )

    def count(dist):
        return sum(jnp.where(there, 1, 0) for _, there in partners(dist))

    barrier = pltpu.get_barrier_semaphore()
    for dev, there in partners(1):
        signal(barrier, dev, there)

    def near_signal(i):
        for dev, there in partners(2**i):
            signal(near_sem.at[i], dev, there)

    def near_wait(i):
        pl.semaphore_wait(near_sem.at[i], count(2**i))

    small = []

    def fetch(src, dst):
        cp = pltpu.make_async_copy(src, dst, lsem.at[len(small)])
        cp.start()
        small.append(cp)
        return cp

    cp_n01 = fetch(nz_h.at[pl.ds(0, 2)], nz.at[pl.ds(0, 2)])
    cp_wf = fetch(wf_h, wf)
    cp_bias = fetch(bias_h, bias)
    cp_obs = fetch(obs_h, obs)
    cp_off = fetch(off_h, off)
    cp_bs = fetch(bs_h, bs)
    cp_fl = fetch(fl_h, fl)

    wcp = [
        (
            pltpu.make_async_copy(wh_h.at[:, c], wh.at[c], wsem.at[0, c]),
            pltpu.make_async_copy(wl_h.at[:, c], wlf.at[c, :, :, pl.ds(0, Z)], wsem.at[1, c]),
        )
        for c in range(CH)
    ]
    for pair in wcp:
        for cp in pair:
            cp.start(priority=1)
    cp_wp = fetch(wp_h, wp)
    cp_n23 = fetch(nz_h.at[pl.ds(2, 2)], nz.at[pl.ds(2, 2)])
    cp_we = fetch(we_h, we)
    cp_weh = fetch(weh_h, weh)

    def link(side, k):
        src, dst = (
            (nz.at[0], rx.at[side, 0]),
            (nz.at[1], rx.at[side, 1]),
            (nz_h.at[2], rx.at[side, 2]),
            (x0.at[side], x0_far.at[side]),
            (rx.at[side, 1], x1_far.at[side]),
        )[k]
        return pltpu.make_async_remote_copy(
            src_ref=src,
            dst_ref=dst,
            send_sem=ssem.at[side, max(k - 2, 0)],
            recv_sem=rsem.at[side, k],
            device_id={"dom": lax.rem(me + 1 - 2 * side + D, D)},
            device_id_type=MESH,
        )

    def within(place):
        return jnp.logical_and(place >= 0, place < D)

    def step_of(side):
        return 1 - 2 * side

    def sends(side, k):
        ahead = within(me + step_of(side))
        return ahead if k < 3 else jnp.logical_and(ahead, within(me - step_of(side)))

    def send(side, k):
        @pl.when(sends(side, k))
        def _():
            link(side, k).start()

    def arrived(k, sides=(0, 1)):
        for side in sides:

            @pl.when(within(me - (1 if k < 3 else 2) * step_of(side)))
            def _():
                link(side, k).wait_recv()

    def all_sent():
        for side in range(2):

            @pl.when(sends(side, 0))
            def _():
                noise = pl.ds(0, 3)
                pltpu.make_async_remote_copy(
                    src_ref=nz_h.at[noise],
                    dst_ref=rx.at[side, noise],
                    send_sem=ssem.at[side, 0],
                    recv_sem=rsem.at[side, 0],
                    device_id={"dom": lax.rem(me + step_of(side) + D, D)},
                    device_id_type=MESH,
                ).wait_send()

            @pl.when(sends(side, 3))
            def _():
                link(side, 3).wait_send()
                link(side, 4).wait_send()

    hz[...] = jnp.zeros_like(hz)
    cz[...] = jnp.zeros_like(cz)
    obs_pad[...] = jnp.zeros_like(obs_pad)
    tpose[X // 16 * 16 :, :] = jnp.zeros((BLK - X // 16 * 16, tpose.shape[1]), BF16)

    cp_bs.wait()
    cp_fl.wait()
    cp_off.wait()
    cp_obs.wait()
    f0, f1, f2 = fl[0] == 1, fl[1] == 1, fl[2] == 1

    around = range(-2, 3)
    place = [lax.rem(me + d + D, D) for d in around]

    def src(t, k, f):
        found = bs[t, place[2]]
        for d, p in zip(around, place):
            found = jnp.where(k - me == d, bs[t, p], found)
        return jnp.where(f, found, k)

    lane = lax.broadcasted_iota(jnp.int32, (1, BLK), 1).astype(F32)
    sub_i = lax.broadcasted_iota(jnp.int32, (BLK, BLK), 0)
    sub = sub_i.astype(F32)

    def flag_mask(f, shape):
        return jnp.broadcast_to(f.astype(jnp.int32), shape) > 0

    def offs(t, k, f):
        away = jnp.broadcast_to(k - me, (1, BLK))
        row = lane
        for d, p in zip(around, place):
            there = off[pl.ds(t, 1), pl.ds(pl.multiple_of(p * BLK, BLK), BLK)].astype(F32)
            row = jnp.where(jnp.logical_and(flag_mask(f, (1, BLK)), away == d), there, row)
        return row

    def onehot(row):
        return jnp.where(sub == row, 1.0, 0.0).astype(BF16)

    def comp(row, hot):
        return mm(jnp.broadcast_to(row, (16, BLK)).astype(BF16), hot)[:1]

    k2 = src(2, me, f2)
    k1 = src(1, k2, f1)
    s1 = src(1, me, f1)
    s0 = src(0, me, f0)
    o0 = src(0, s1, f0)
    k0 = src(0, k1, f0)
    hot_q = onehot(offs(2, me, f2))
    hot_r = onehot(comp(offs(1, k2, f1), hot_q))
    hot_s = onehot(comp(offs(0, k1, f0), hot_r))
    hot_o1 = onehot(offs(1, me, f1))
    hot_o0 = onehot(comp(offs(0, s1, f0), hot_o1))
    hot_c0 = onehot(offs(0, me, f0))
    def pick(t, k):
        d = jnp.broadcast_to(k - me, (Z, BLK))
        out = jnp.where(d < 0, rx[0, t], jnp.where(d > 0, rx[1, t], nz[t]))
        if t != 1:
            return out
        return jnp.where(d == -2, x1_far[0], jnp.where(d == 2, x1_far[1], out))

    def latent_0(k, hot, far=True):
        lat = mean0 + std0 * pick(0, k)
        if far:
            d = jnp.broadcast_to(k - me, (Z, BLK))
            lat = jnp.where(d == -2, x0_far[0].astype(F32), lat)
            lat = jnp.where(d == 2, x0_far[1].astype(F32), lat)
        return mm(lat.astype(BF16), hot).astype(BF16)

    def gather3(x, hot):
        hi, mid, lo = split3(x)
        out = mm(jnp.concatenate([hi, mid, lo], axis=0), hot)
        return out[:BLK] + out[BLK : 2 * BLK] + out[2 * BLK :]

    steps = obs.shape[0] - 1
    obs_pad[0 : steps + 1, 0:X] = obs[...].astype(F32)
    obs_t = jnp.transpose(obs_pad[...])

    def frame_col(t):
        return jnp.broadcast_to(obs_t[:, t : t + 1], (BLK, BLK))

    ones = jnp.logical_and(sub_i >= 96, sub_i < 99)
    tails = [jnp.where(ones, 1.0, frame_col(t)).astype(BF16) for t in range(steps)]

    cp_wf.wait()
    cp_bias.wait()
    tpose[0:X, :] = wf[...]
    hi, mid, lo = (p.astype(F32) for p in split3(bias[...]))
    r16 = lax.broadcasted_iota(jnp.int32, (16, bias.shape[1]), 0)
    tpose[96:112, :] = jnp.where(
        r16 == 0, hi, jnp.where(r16 == 1, mid, jnp.where(r16 == 2, lo, 0.0))
    ).astype(BF16)
    for c in range(CH):
        for g in range(4):
            for i in range(0, HC, BLK):
                rows = g * H + c * HC + i
                wlf[c, g, i : i + BLK, Z : Z + BLK] = jnp.transpose(
                    tpose[:, rows : rows + BLK]
                )

    pl.semaphore_wait(barrier, count(1))
    cp_n01.wait()
    for t in range(3):
        for side in range(2):
            send(side, t)
    near_signal(0)

    def run_layer(gates, elem, hooks={}):
        bufs = (ga, gb)
        for c in range(CH):
            hooks.get(c, lambda: None)()
            val = gates(c)
            bufs[c % 2][:, : val.shape[1]] = val
            if c:
                elem(c - 1, bufs[(c - 1) % 2])
        elem(CH - 1, bufs[(CH - 1) % 2])

    def elem_of(n, old, h_out, c_out):
        def elem(c, buf):
            rows = slice(c * HC, (c + 1) * HC)
            h, s = cell_update(buf[:, :n], old[rows, :n], HC)
            h_out[rows, :n] = h
            if c_out is not None:
                c_out[rows, :n] = s

        return elem

    def moments(h):
        return mm(wp[:Z, :], h), jnp.exp(0.5 * jnp.tanh(mm(wp[Z:, :], h)))

    def increment(t, lat, h):
        pred = mm(we[...], lat) + mm(weh[...], h)
        target = frame_col(t + 1)[:X]
        return jnp.sum(pred * (target - 0.5 * pred), axis=0, keepdims=True)

    lat_tail0 = jnp.concatenate([jnp.zeros((Z, BLK), BF16), tails[0]], axis=0)

    def w_h(c):
        return wh[c].reshape(4 * HC, H)

    def w_lf(c):
        return wlf[c].reshape(4 * HC, Z + BLK)

    def weights_here(c):
        for pair in wcp[c : c + 2]:
            for cp in pair:
                cp.wait()

    def third():
        weights_here(4)
        near_wait(0)
        near_signal(1)

    def fourth():
        weights_here(6)
        cp_wp.wait()
        cp_n23.wait()
        cp_we.wait()
        cp_weh.wait()

    run_layer(
        lambda c: mm(w_h(c), hz[...]) + mm(w_lf(c), lat_tail0),
        elem_of(BLK, cz, h1, c1),
        {0: lambda: weights_here(0), 2: lambda: weights_here(2), 4: third, 6: fourth},
    )
    mean0, std0 = moments(h1[...])

    def relay_0(side):
        arrived(0, (side,))
        x0[side] = (mean0 + std0 * rx[side, 0]).astype(BF16)
        send(side, 3)

    first = jnp.where(lax.rem(me, 4) == 0, 1, 0)
    relay_0(first)
    for c in range(2):
        g1[c] = mm(w_h(c), h1[...])
    relay_0(1 - first)
    near_wait(1)
    near_signal(2)
    lat_c = latent_0(s0, hot_c0, False)
    tail_c = jnp.concatenate([lat_c, tails[1]], axis=0)
    lw0 = increment(0, (mean0 + std0 * nz[0]).astype(BF16), h1[...])

    def gates_c(c):
        if c > 1:
            g1[c] = mm(w_h(c), h1[...])
        return g1[c] + mm(w_lf(c), tail_c)

    def relay_1():
        arrived(1)
        send(0, 4)
        send(1, 4)

    run_layer(gates_c, elem_of(BLK, c1, hc, None), {4: relay_1})
    near_wait(2)
    arrived(3)
    near_signal(3)
    mean_c, std_c = moments(hc[...])
    inc_c = increment(1, (mean_c + std_c * nz[1]).astype(BF16), hc[...])
    lw1 = jnp.where(flag_mask(f0, (1, BLK)), 0.0, lw0) + inc_c

    lat_o = latent_0(o0, hot_o0)
    lat_l = latent_0(k0, hot_s)
    tail_ol = jnp.concatenate(
        [
            jnp.concatenate([lat_o, lat_l], axis=1),
            jnp.concatenate([tails[1], tails[1]], axis=1),
        ],
        axis=0,
    )

    def gates1(c):
        g = g1[c]
        return jnp.concatenate([g, g], axis=1) + mm(w_lf(c), tail_ol)

    def elem1(c, buf):
        rows = slice(c * HC, (c + 1) * HC)
        old = c1[rows, :]
        h, s = cell_update(buf[...], jnp.concatenate([old, old], axis=1), HC)
        h2[rows, :] = h
        c2[rows, :] = s

    run_layer(gates1, elem1)
    m1, sd1 = moments(h2[...])
    early = CH // 2
    late = early + 2
    for c in range(early):
        gc[c] = mm(w_h(c), h2[...])
    near_wait(3)
    arrived(4)
    arrived(2)
    near_signal(4)
    n1_o = gather3(pick(1, s1), hot_o1)
    n1_l = gather3(pick(1, k1), hot_r)
    for c in range(early, late):
        gc[c] = mm(w_h(c), h2[...])
    lat1 = (m1 + sd1 * jnp.concatenate([n1_o, n1_l], axis=1)).astype(BF16)

    tail2 = jnp.concatenate(
        [lat1, jnp.concatenate([tails[2], tails[2]], axis=1)], axis=0
    )

    def gates2(c):
        part = gc[c] if c < late else mm(w_h(c), h2[...])
        return part + mm(w_lf(c), tail2)

    run_layer(gates2, elem_of(2 * BLK, c2, h3, c3))
    m2, sd2 = moments(h3[...])
    for c in range(2):
        g1[c] = mm(w_h(c), h3[:, BLK:])
    n2_l = gather3(pick(2, k2), hot_q)
    lat2 = (m2 + sd2 * jnp.concatenate([nz[2], n2_l], axis=1)).astype(BF16)
    tail3 = jnp.concatenate([lat2[:, BLK:], tails[3]], axis=0)

    def gates3(c):
        part = g1[c] if c < 2 else mm(w_h(c), h3[:, BLK:])
        return part + mm(w_lf(c), tail3)

    def elem3(c, buf):
        rows = slice(c * HC, (c + 1) * HC)
        h, _ = cell_update(buf[:, :BLK], c3[rows, BLK:], HC)
        h4[rows, :] = h

    run_layer(gates3, elem3)
    inc2 = increment(2, lat2[:, :BLK], h3[:, :BLK])
    lw2 = jnp.where(flag_mask(f1, (1, BLK)), 0.0, lw1) + inc2
    m3, sd3 = moments(h4[...])
    lat3 = (m3 + sd3 * nz[3]).astype(BF16)
    lw3 = jnp.where(flag_mask(f2, (1, BLK)), 0.0, lw2) + increment(3, lat3, h4[...])

    def lse(lw):
        peak = jnp.max(lw, axis=1, keepdims=True)
        return peak + jnp.log(jnp.sum(jnp.exp(lw - peak), axis=1, keepdims=True))

    lane_i = lax.broadcasted_iota(jnp.int32, (1, BLK), 1)
    row = jnp.zeros((1, BLK), F32)
    for t, lw in enumerate((lw0, lw1, lw2, lw3)):
        row = jnp.where(lane_i == t, lse(lw), row)
    lse_row[...] = row
    lse_all[pl.ds(me, 1)] = row[None]
    used = lane_i == steps - 1
    for t, f in enumerate((f0, f1, f2)):
        used = jnp.logical_or(used, jnp.logical_and(lane_i == t, flag_mask(f, (1, BLK))))
    used_o[...] = jnp.where(used, 1.0, 0.0)
    near_wait(4)
    for d in range(1, D):
        pltpu.make_async_remote_copy(
            src_ref=lse_row,
            dst_ref=lse_all.at[me],
            send_sem=as_sem,
            recv_sem=ar_sem,
            device_id={"dom": lax.rem(me + d, D)},
            device_id_type=MESH,
        ).start()
    all_sent()
    others = lse_all.at[pl.ds(0, D - 1)]
    every = pltpu.make_async_remote_copy(
        src_ref=others,
        dst_ref=others,
        send_sem=as_sem,
        recv_sem=ar_sem,
        device_id={"dom": right},
        device_id_type=MESH,
    )
    every.wait_recv()
    every.wait_send()


def finish(h_ref, lse_all, used, hid_o, bnd_o, sem):
    out_cp = pltpu.make_async_copy(h_ref, hid_o, sem)
    out_cp.start()
    every = lse_all[...]
    peak = jnp.max(every, axis=0)
    total = jnp.log(jnp.sum(jnp.exp(every - peak[None]), axis=0))
    level = peak + total - math.log(every.shape[0] * BLK)
    bnd_o[...] = jnp.sum(jnp.where(used[...] > 0, level, 0.0), axis=1, keepdims=True)
    out_cp.wait()


def body(
    observed,
    latent_noise,
    w_hidden,
    w_latent,
    w_frame,
    gate_bias,
    w_prior,
    w_emit,
    w_emit_hidden,
    block_source,
    inner_offset,
    resample_flags,
):
    D = lax.axis_size("dom")
    steps, Z, n = latent_noise.shape
    H = w_hidden.shape[1]
    X = w_emit.shape[0]
    G = 4 * H // CH
    V = pltpu.VMEM
    DMA = pltpu.SemaphoreType.DMA
    pinned = [
        pltpu.with_memory_space_constraint(x, pltpu.HBM)
        for x in (
            observed,
            latent_noise,
            w_hidden.reshape(4, CH, H // CH, H),
            w_latent.reshape(4, CH, H // CH, Z),
            w_frame,
            gate_bias.reshape(1, -1),
            w_prior,
            w_emit,
            w_emit_hidden,
            block_source,
            inner_offset,
            resample_flags,
        )
    ]
    last_hidden, lse_all, used = pl.pallas_call(
        functools.partial(kernel, D),
        out_shape=(
            jax.ShapeDtypeStruct((H, n), BF16),
            jax.ShapeDtypeStruct((D, 1, BLK), F32),
            jax.ShapeDtypeStruct((1, BLK), F32),
        ),
        in_specs=[pl.BlockSpec(memory_space=pltpu.HBM)] * 12,
        out_specs=(pl.BlockSpec(memory_space=pltpu.VMEM),) * 3,
        scratch_shapes=[
            V((CH, 4, H // CH, H), BF16),
            V((CH, 4, H // CH, Z + BLK), BF16),
            V((X, 4 * H), BF16),
            V((BLK, 4 * H), BF16),
            V((1, 4 * H), F32),
            V((2 * Z, H), BF16),
            V((X, Z), BF16),
            V((X, H), BF16),
            V((steps + 1, X), BF16),
            V((BLK, BLK), F32),
            V((steps, Z, n), F32),
            V(inner_offset.shape, jnp.int32),
            pltpu.SMEM(block_source.shape, jnp.int32),
            pltpu.SMEM(resample_flags.shape, jnp.int32),
            V((2, 3, Z, n), F32),
            V((2, Z, n), BF16),
            V((2, Z, n), BF16),
            V((2, Z, n), F32),
            V((CH, G, n), F32),
            V((G, 2 * n), F32),
            V((G, 2 * n), F32),
            V((CH // 2 + 2, G, 2 * n), F32),
            V((H, n), BF16),
            V((H, n), BF16),
            V((H, n), BF16),
            V((H, n), BF16),
            V((H, n), BF16),
            V((H, 2 * n), BF16),
            V((H, 2 * n), BF16),
            V((H, 2 * n), BF16),
            V((H, 2 * n), BF16),
            V((1, BLK), F32),
            DMA((2, CH)),
            DMA((11,)),
            DMA((2, 3)),
            DMA((2, 5)),
            DMA,
            DMA,
            pltpu.SemaphoreType.REGULAR((5,)),
        ],
        compiler_params=pltpu.CompilerParams(
            collective_id=0, has_side_effects=True, vmem_limit_bytes=32 * 2**20
        ),
        name="filter_steps",
    )(*pinned)
    hidden, bound = pl.pallas_call(
        finish,
        out_shape=(
            jax.ShapeDtypeStruct((H, n), BF16),
            jax.ShapeDtypeStruct((1, 1), F32),
        ),
        in_specs=[pl.BlockSpec(memory_space=pltpu.VMEM)] * 3,
        out_specs=(
            pl.BlockSpec(memory_space=pl.ANY),
            pl.BlockSpec(memory_space=pltpu.VMEM),
        ),
        scratch_shapes=[DMA],
        compiler_params=pltpu.CompilerParams(vmem_limit_bytes=2 * 2**20),
        name="finish",
    )(last_hidden, lse_all, used)
    return hidden, bound.reshape(1)


def solution(mesh):
    in_specs = (
        P("seq", None),
        P(None, None, ("seq", "dom")),
        P(),
        P(),
        P(),
        P(),
        P(),
        P(),
        P(),
        P("seq", None),
        P("seq", None),
        P(),
    )
    out_specs = (P(None, ("seq", "dom")), P("seq"))
    return jax.shard_map(body, mesh=mesh, in_specs=in_specs, out_specs=out_specs, check_vma=False)
```

```python
import functools
import math

import jax
import jax.numpy as jnp
from jax import lax
from jax.experimental import pallas as pl
from jax.experimental.pallas import tpu as pltpu
from jax.sharding import PartitionSpec as P

BLK = 128
F32 = jnp.float32
BF16 = jnp.bfloat16
MESH = pl.DeviceIdType.MESH
CH = 8


def mm(a, b):
    return jnp.dot(a, b, preferred_element_type=F32)


def sig(x):
    return 0.5 * jnp.tanh(0.5 * x) + 0.5


def cell_update(gates, old, n):
    in_gate = sig(gates[:n])
    forget = sig(gates[n : 2 * n])
    cand = jnp.tanh(gates[2 * n : 3 * n])
    out_gate = sig(gates[3 * n :])
    fresh = forget * old.astype(F32) + in_gate * cand
    return (out_gate * jnp.tanh(fresh)).astype(BF16), fresh.astype(BF16)


def split3(x):
    hi = x.astype(BF16)
    rest = x - hi.astype(F32)
    mid = rest.astype(BF16)
    return hi, mid, (rest - mid.astype(F32)).astype(BF16)


def kernel(
    D,
    obs_h,
    nz_h,
    wh_h,
    wl_h,
    wf_h,
    bias_h,
    wp_h,
    we_h,
    weh_h,
    bs_h,
    off_h,
    fl_h,
    h4,
    lse_all,
    used_o,
    wh,
    wlf,
    wf,
    tpose,
    bias,
    wp,
    we,
    weh,
    obs,
    obs_pad,
    nz,
    off,
    bs,
    fl,
    rx,
    x0,
    x0_far,
    x1_far,
    g1,
    ga,
    gb,
    gc,
    hz,
    cz,
    h1,
    c1,
    hc,
    h2,
    c2,
    h3,
    c3,
    lse_row,
    wsem,
    lsem,
    ssem,
    rsem,
    as_sem,
    ar_sem,
    near_sem,
):
    H = wh.shape[3]
    Z = we.shape[1]
    X = we.shape[0]
    HC = H // CH
    me = lax.axis_index("dom")
    right = lax.rem(me + 1, D)
    left = lax.rem(me + D - 1, D)

    def signal(sem, dev, there):
        @pl.when(there)
        def _():
            pl.semaphore_signal(sem, inc=1, device_id={"dom": dev}, device_id_type=MESH)

    def partners(dist):
        return (
            (lax.rem(me + dist, D), me + dist < D),
            (lax.rem(me + D - dist, D), me >= dist),
        )

    def count(dist):
        return sum(jnp.where(there, 1, 0) for _, there in partners(dist))

    barrier = pltpu.get_barrier_semaphore()
    for dev, there in partners(1):
        signal(barrier, dev, there)

    def near_signal(i):
        for dev, there in partners(2**i):
            signal(near_sem.at[i], dev, there)

    def near_wait(i):
        pl.semaphore_wait(near_sem.at[i], count(2**i))

    small = []

    def fetch(src, dst):
        cp = pltpu.make_async_copy(src, dst, lsem.at[len(small)])
        cp.start()
        small.append(cp)
        return cp

    cp_n01 = fetch(nz_h.at[pl.ds(0, 2)], nz.at[pl.ds(0, 2)])
    cp_wf = fetch(wf_h, wf)
    cp_bias = fetch(bias_h, bias)
    cp_obs = fetch(obs_h, obs)
    cp_off = fetch(off_h, off)
    cp_bs = fetch(bs_h, bs)
    cp_fl = fetch(fl_h, fl)

    wcp = [
        (
            pltpu.make_async_copy(wh_h.at[:, c], wh.at[c], wsem.at[0, c]),
            pltpu.make_async_copy(wl_h.at[:, c], wlf.at[c, :, :, pl.ds(0, Z)], wsem.at[1, c]),
        )
        for c in range(CH)
    ]
    def start_weights(c, n):
        for pair in wcp[c : c + n]:
            for cp in pair:
                cp.start(priority=1)

    start_weights(0, 2)
    cp_wp = fetch(wp_h, wp)
    cp_n23 = fetch(nz_h.at[pl.ds(2, 2)], nz.at[pl.ds(2, 2)])
    cp_we = fetch(we_h, we)
    cp_weh = fetch(weh_h, weh)

    def link(side, k):
        src, dst = (
            (nz.at[0], rx.at[side, 0]),
            (nz.at[1], rx.at[side, 1]),
            (nz_h.at[2], rx.at[side, 2]),
            (x0.at[side], x0_far.at[side]),
            (rx.at[side, 1], x1_far.at[side]),
        )[k]
        return pltpu.make_async_remote_copy(
            src_ref=src,
            dst_ref=dst,
            send_sem=ssem.at[side, max(k - 2, 0)],
            recv_sem=rsem.at[side, k],
            device_id={"dom": lax.rem(me + 1 - 2 * side + D, D)},
            device_id_type=MESH,
        )

    def within(place):
        return jnp.logical_and(place >= 0, place < D)

    def step_of(side):
        return 1 - 2 * side

    def sends(side, k):
        ahead = within(me + step_of(side))
        return ahead if k < 3 else jnp.logical_and(ahead, within(me - step_of(side)))

    def send(side, k):
        @pl.when(sends(side, k))
        def _():
            link(side, k).start()

    def arrived(k, sides=(0, 1)):
        for side in sides:

            @pl.when(within(me - (1 if k < 3 else 2) * step_of(side)))
            def _():
                link(side, k).wait_recv()

    def all_sent():
        for side in range(2):

            @pl.when(sends(side, 0))
            def _():
                noise = pl.ds(0, 3)
                pltpu.make_async_remote_copy(
                    src_ref=nz_h.at[noise],
                    dst_ref=rx.at[side, noise],
                    send_sem=ssem.at[side, 0],
                    recv_sem=rsem.at[side, 0],
                    device_id={"dom": lax.rem(me + step_of(side) + D, D)},
                    device_id_type=MESH,
                ).wait_send()

            @pl.when(sends(side, 3))
            def _():
                link(side, 3).wait_send()
                link(side, 4).wait_send()

    hz[...] = jnp.zeros_like(hz)
    cz[...] = jnp.zeros_like(cz)
    obs_pad[...] = jnp.zeros_like(obs_pad)
    tpose[X // 16 * 16 :, :] = jnp.zeros((BLK - X // 16 * 16, tpose.shape[1]), BF16)

    start_weights(2, 6)
    cp_bs.wait()
    cp_fl.wait()
    cp_off.wait()
    cp_obs.wait()
    f0, f1, f2 = fl[0] == 1, fl[1] == 1, fl[2] == 1

    around = range(-2, 3)
    place = [lax.rem(me + d + D, D) for d in around]

    def src(t, k, f):
        found = bs[t, place[2]]
        for d, p in zip(around, place):
            found = jnp.where(k - me == d, bs[t, p], found)
        return jnp.where(f, found, k)

    lane = lax.broadcasted_iota(jnp.int32, (1, BLK), 1).astype(F32)
    sub_i = lax.broadcasted_iota(jnp.int32, (BLK, BLK), 0)
    sub = sub_i.astype(F32)

    def flag_mask(f, shape):
        return jnp.broadcast_to(f.astype(jnp.int32), shape) > 0

    def offs(t, k, f):
        away = jnp.broadcast_to(k - me, (1, BLK))
        row = lane
        for d, p in zip(around, place):
            there = off[pl.ds(t, 1), pl.ds(pl.multiple_of(p * BLK, BLK), BLK)].astype(F32)
            row = jnp.where(jnp.logical_and(flag_mask(f, (1, BLK)), away == d), there, row)
        return row

    def onehot(row):
        return jnp.where(sub == row, 1.0, 0.0).astype(BF16)

    def comp(row, hot):
        return mm(jnp.broadcast_to(row, (16, BLK)).astype(BF16), hot)[:1]

    k2 = src(2, me, f2)
    k1 = src(1, k2, f1)
    s1 = src(1, me, f1)
    s0 = src(0, me, f0)
    o0 = src(0, s1, f0)
    k0 = src(0, k1, f0)
    hot_q = onehot(offs(2, me, f2))
    hot_r = onehot(comp(offs(1, k2, f1), hot_q))
    hot_s = onehot(comp(offs(0, k1, f0), hot_r))
    hot_o1 = onehot(offs(1, me, f1))
    hot_o0 = onehot(comp(offs(0, s1, f0), hot_o1))
    hot_c0 = onehot(offs(0, me, f0))
    def pick(t, k):
        d = jnp.broadcast_to(k - me, (Z, BLK))
        out = jnp.where(d < 0, rx[0, t], jnp.where(d > 0, rx[1, t], nz[t]))
        if t != 1:
            return out
        return jnp.where(d == -2, x1_far[0], jnp.where(d == 2, x1_far[1], out))

    def latent_0(k, hot, far=True):
        lat = mean0 + std0 * pick(0, k)
        if far:
            d = jnp.broadcast_to(k - me, (Z, BLK))
            lat = jnp.where(d == -2, x0_far[0].astype(F32), lat)
            lat = jnp.where(d == 2, x0_far[1].astype(F32), lat)
        return mm(lat.astype(BF16), hot).astype(BF16)

    def gather3(x, hot):
        hi, mid, lo = split3(x)
        out = mm(jnp.concatenate([hi, mid, lo], axis=0), hot)
        return out[:BLK] + out[BLK : 2 * BLK] + out[2 * BLK :]

    steps = obs.shape[0] - 1
    obs_pad[0 : steps + 1, 0:X] = obs[...].astype(F32)
    obs_t = jnp.transpose(obs_pad[...])

    def frame_col(t):
        return jnp.broadcast_to(obs_t[:, t : t + 1], (BLK, BLK))

    ones = jnp.logical_and(sub_i >= 96, sub_i < 99)
    tails = [jnp.where(ones, 1.0, frame_col(t)).astype(BF16) for t in range(steps)]

    cp_wf.wait()
    cp_bias.wait()
    tpose[0:X, :] = wf[...]
    hi, mid, lo = (p.astype(F32) for p in split3(bias[...]))
    r16 = lax.broadcasted_iota(jnp.int32, (16, bias.shape[1]), 0)
    tpose[96:112, :] = jnp.where(
        r16 == 0, hi, jnp.where(r16 == 1, mid, jnp.where(r16 == 2, lo, 0.0))
    ).astype(BF16)
    for c in range(CH):
        for g in range(4):
            for i in range(0, HC, BLK):
                rows = g * H + c * HC + i
                wlf[c, g, i : i + BLK, Z : Z + BLK] = jnp.transpose(
                    tpose[:, rows : rows + BLK]
                )

    pl.semaphore_wait(barrier, count(1))
    cp_n01.wait()
    for t in range(3):
        for side in range(2):
            send(side, t)
    near_signal(0)

    def run_layer(gates, elem, hooks={}):
        bufs = (ga, gb)
        for c in range(CH):
            hooks.get(c, lambda: None)()
            val = gates(c)
            bufs[c % 2][:, : val.shape[1]] = val
            if c:
                elem(c - 1, bufs[(c - 1) % 2])
        elem(CH - 1, bufs[(CH - 1) % 2])

    def elem_of(n, old, h_out, c_out):
        def elem(c, buf):
            rows = slice(c * HC, (c + 1) * HC)
            h, s = cell_update(buf[:, :n], old[rows, :n], HC)
            h_out[rows, :n] = h
            if c_out is not None:
                c_out[rows, :n] = s

        return elem

    def moments(h):
        return mm(wp[:Z, :], h), jnp.exp(0.5 * jnp.tanh(mm(wp[Z:, :], h)))

    def increment(t, lat, h):
        pred = mm(we[...], lat) + mm(weh[...], h)
        target = frame_col(t + 1)[:X]
        return jnp.sum(pred * (target - 0.5 * pred), axis=0, keepdims=True)

    lat_tail0 = jnp.concatenate([jnp.zeros((Z, BLK), BF16), tails[0]], axis=0)

    def halves(c, first, tail=None):
        out = []
        for g in (0, 2):
            rows = slice(g * HC, (g + 2) * HC)
            val = first(g, rows)
            if tail is not None:
                val = val + mm(wlf[c, g : g + 2].reshape(2 * HC, Z + BLK), tail)
            out.append(val)
        return jnp.concatenate(out, axis=0)

    def product(c, state, tail=None):
        def first(g, rows):
            return mm(wh[c, g : g + 2].reshape(2 * HC, H), state)

        return halves(c, first, tail)

    def with_tail(c, ref, tail, wide=False):
        def first(g, rows):
            part = ref[c, rows, :]
            return jnp.concatenate([part, part], axis=1) if wide else part

        return halves(c, first, tail)

    def weights_here(c, n):
        for pair in wcp[c : c + n]:
            for cp in pair:
                cp.wait()

    def third():
        weights_here(4, 4)
        near_wait(0)
        near_signal(1)
        cp_wp.wait()
        cp_n23.wait()
        cp_we.wait()
        cp_weh.wait()

    run_layer(
        lambda c: product(c, hz[...], lat_tail0),
        elem_of(BLK, cz, h1, c1),
        {0: lambda: weights_here(0, 2), 2: lambda: weights_here(2, 2), 4: third},
    )
    mean0, std0 = moments(h1[...])

    def relay_0(side):
        arrived(0, (side,))
        x0[side] = (mean0 + std0 * rx[side, 0]).astype(BF16)
        send(side, 3)

    first = jnp.where(lax.rem(me, 4) == 0, 1, 0)
    relay_0(first)
    inner = jnp.logical_or(lax.rem(me, 4) == 1, lax.rem(me, 4) == 2)

    @pl.when(inner)
    def _():
        relay_0(1 - first)

    for c in range(2):
        g1[c] = product(c, h1[...])

    @pl.when(jnp.logical_not(inner))
    def _():
        relay_0(1 - first)

    near_wait(1)
    near_signal(2)
    lat_c = latent_0(s0, hot_c0, False)
    tail_c = jnp.concatenate([lat_c, tails[1]], axis=0)
    lw0 = increment(0, (mean0 + std0 * nz[0]).astype(BF16), h1[...])

    def gates_c(c):
        if c > 1:
            g1[c] = product(c, h1[...])
        return with_tail(c, g1, tail_c)

    def relay_1():
        arrived(1)
        send(0, 4)
        send(1, 4)

    run_layer(gates_c, elem_of(BLK, c1, hc, None), {4: relay_1})
    near_wait(2)
    arrived(3)
    near_signal(3)
    mean_c, std_c = moments(hc[...])
    inc_c = increment(1, (mean_c + std_c * nz[1]).astype(BF16), hc[...])
    lw1 = jnp.where(flag_mask(f0, (1, BLK)), 0.0, lw0) + inc_c

    lat_o = latent_0(o0, hot_o0)
    lat_l = latent_0(k0, hot_s)
    tail_ol = jnp.concatenate(
        [
            jnp.concatenate([lat_o, lat_l], axis=1),
            jnp.concatenate([tails[1], tails[1]], axis=1),
        ],
        axis=0,
    )

    def gates1(c):
        return with_tail(c, g1, tail_ol, True)

    def elem1(c, buf):
        rows = slice(c * HC, (c + 1) * HC)
        old = c1[rows, :]
        h, s = cell_update(buf[...], jnp.concatenate([old, old], axis=1), HC)
        h2[rows, :] = h
        c2[rows, :] = s

    run_layer(gates1, elem1)
    m1, sd1 = moments(h2[...])
    early, late = 2, 4
    for c in range(early):
        gc[c] = product(c, h2[...])
    near_wait(3)
    arrived(4)
    arrived(2)
    near_signal(4)
    n1_o = gather3(pick(1, s1), hot_o1)
    n1_l = gather3(pick(1, k1), hot_r)
    for c in range(early, late):
        gc[c] = product(c, h2[...])
    lat1 = (m1 + sd1 * jnp.concatenate([n1_o, n1_l], axis=1)).astype(BF16)

    tail2 = jnp.concatenate(
        [lat1, jnp.concatenate([tails[2], tails[2]], axis=1)], axis=0
    )

    def gates2(c):
        if c < late:
            return with_tail(c, gc, tail2)
        return product(c, h2[...], tail2)

    run_layer(gates2, elem_of(2 * BLK, c2, h3, c3))
    m2, sd2 = moments(h3[...])
    for c in range(2):
        g1[c] = product(c, h3[:, BLK:])
    n2_l = gather3(pick(2, k2), hot_q)
    lat2 = (m2 + sd2 * jnp.concatenate([nz[2], n2_l], axis=1)).astype(BF16)
    tail3 = jnp.concatenate([lat2[:, BLK:], tails[3]], axis=0)

    def gates3(c):
        if c < 2:
            return with_tail(c, g1, tail3)
        return product(c, h3[:, BLK:], tail3)

    def elem3(c, buf):
        rows = slice(c * HC, (c + 1) * HC)
        h, _ = cell_update(buf[:, :BLK], c3[rows, BLK:], HC)
        h4[rows, :] = h

    run_layer(gates3, elem3)
    inc2 = increment(2, lat2[:, :BLK], h3[:, :BLK])
    lw2 = jnp.where(flag_mask(f1, (1, BLK)), 0.0, lw1) + inc2
    m3, sd3 = moments(h4[...])
    lat3 = (m3 + sd3 * nz[3]).astype(BF16)
    lw3 = jnp.where(flag_mask(f2, (1, BLK)), 0.0, lw2) + increment(3, lat3, h4[...])

    def lse(lw):
        peak = jnp.max(lw, axis=1, keepdims=True)
        return peak + jnp.log(jnp.sum(jnp.exp(lw - peak), axis=1, keepdims=True))

    lane_i = lax.broadcasted_iota(jnp.int32, (1, BLK), 1)
    row = jnp.zeros((1, BLK), F32)
    for t, lw in enumerate((lw0, lw1, lw2, lw3)):
        row = jnp.where(lane_i == t, lse(lw), row)
    lse_row[...] = row
    lse_all[pl.ds(me, 1)] = row[None]
    used = lane_i == steps - 1
    for t, f in enumerate((f0, f1, f2)):
        used = jnp.logical_or(used, jnp.logical_and(lane_i == t, flag_mask(f, (1, BLK))))
    used_o[...] = jnp.where(used, 1.0, 0.0)
    near_wait(4)
    for d in range(1, D):
        pltpu.make_async_remote_copy(
            src_ref=lse_row,
            dst_ref=lse_all.at[me],
            send_sem=as_sem,
            recv_sem=ar_sem,
            device_id={"dom": lax.rem(me + d, D)},
            device_id_type=MESH,
        ).start()
    all_sent()
    others = lse_all.at[pl.ds(0, D - 1)]
    every = pltpu.make_async_remote_copy(
        src_ref=others,
        dst_ref=others,
        send_sem=as_sem,
        recv_sem=ar_sem,
        device_id={"dom": right},
        device_id_type=MESH,
    )
    every.wait_recv()
    every.wait_send()


def finish(h_ref, lse_all, used, hid_o, bnd_o, bnd, sem):
    out_cp = pltpu.make_async_copy(h_ref, hid_o, sem.at[0])
    out_cp.start()
    every = lse_all[...]
    peak = jnp.max(every, axis=0)
    total = jnp.log(jnp.sum(jnp.exp(every - peak[None]), axis=0))
    level = peak + total - math.log(every.shape[0] * BLK)
    bnd[...] = jnp.sum(jnp.where(used[...] > 0, level, 0.0), axis=1, keepdims=True)
    bnd_cp = pltpu.make_async_copy(bnd, bnd_o, sem.at[1])
    bnd_cp.start()
    out_cp.wait()
    bnd_cp.wait()


def body(
    observed,
    latent_noise,
    w_hidden,
    w_latent,
    w_frame,
    gate_bias,
    w_prior,
    w_emit,
    w_emit_hidden,
    block_source,
    inner_offset,
    resample_flags,
):
    D = lax.axis_size("dom")
    steps, Z, n = latent_noise.shape
    H = w_hidden.shape[1]
    X = w_emit.shape[0]
    G = 4 * H // CH
    V = pltpu.VMEM
    DMA = pltpu.SemaphoreType.DMA
    pinned = [
        pltpu.with_memory_space_constraint(x, pltpu.HBM)
        for x in (
            observed,
            latent_noise,
            w_hidden.reshape(4, CH, H // CH, H),
            w_latent.reshape(4, CH, H // CH, Z),
            w_frame,
            gate_bias.reshape(1, -1),
            w_prior,
            w_emit,
            w_emit_hidden,
            block_source,
            inner_offset,
            resample_flags,
        )
    ]
    last_hidden, lse_all, used = pl.pallas_call(
        functools.partial(kernel, D),
        out_shape=(
            jax.ShapeDtypeStruct((H, n), BF16),
            jax.ShapeDtypeStruct((D, 1, BLK), F32),
            jax.ShapeDtypeStruct((1, BLK), F32),
        ),
        in_specs=[pl.BlockSpec(memory_space=pltpu.HBM)] * 12,
        out_specs=(pl.BlockSpec(memory_space=pltpu.VMEM),) * 3,
        scratch_shapes=[
            V((CH, 4, H // CH, H), BF16),
            V((CH, 4, H // CH, Z + BLK), BF16),
            V((X, 4 * H), BF16),
            V((BLK, 4 * H), BF16),
            V((1, 4 * H), F32),
            V((2 * Z, H), BF16),
            V((X, Z), BF16),
            V((X, H), BF16),
            V((steps + 1, X), BF16),
            V((BLK, BLK), F32),
            V((steps, Z, n), F32),
            V(inner_offset.shape, jnp.int32),
            pltpu.SMEM(block_source.shape, jnp.int32),
            pltpu.SMEM(resample_flags.shape, jnp.int32),
            V((2, 3, Z, n), F32),
            V((2, Z, n), BF16),
            V((2, Z, n), BF16),
            V((2, Z, n), F32),
            V((CH, G, n), F32),
            V((G, 2 * n), F32),
            V((G, 2 * n), F32),
            V((CH // 2 + 2, G, 2 * n), F32),
            V((H, n), BF16),
            V((H, n), BF16),
            V((H, n), BF16),
            V((H, n), BF16),
            V((H, n), BF16),
            V((H, 2 * n), BF16),
            V((H, 2 * n), BF16),
            V((H, 2 * n), BF16),
            V((H, 2 * n), BF16),
            V((1, BLK), F32),
            DMA((2, CH)),
            DMA((11,)),
            DMA((2, 3)),
            DMA((2, 5)),
            DMA,
            DMA,
            pltpu.SemaphoreType.REGULAR((5,)),
        ],
        compiler_params=pltpu.CompilerParams(
            collective_id=0, has_side_effects=True, vmem_limit_bytes=32 * 2**20
        ),
        name="filter_steps",
    )(*pinned)
    hidden, bound = pl.pallas_call(
        finish,
        out_shape=(
            jax.ShapeDtypeStruct((H, n), BF16),
            jax.ShapeDtypeStruct((1, 1), F32),
        ),
        in_specs=[pl.BlockSpec(memory_space=pltpu.VMEM)] * 3,
        out_specs=(pl.BlockSpec(memory_space=pl.ANY),) * 2,
        scratch_shapes=[V((1, 1), F32), DMA((2,))],
        compiler_params=pltpu.CompilerParams(vmem_limit_bytes=2 * 2**20),
        name="finish",
    )(last_hidden, lse_all, used)
    return hidden, bound.reshape(1)


def solution(mesh):
    in_specs = (
        P("seq", None),
        P(None, None, ("seq", "dom")),
        P(),
        P(),
        P(),
        P(),
        P(),
        P(),
        P(),
        P("seq", None),
        P("seq", None),
        P(),
    )
    out_specs = (P(None, ("seq", "dom")), P("seq"))
    return jax.shard_map(body, mesh=mesh, in_specs=in_specs, out_specs=out_specs, check_vma=False)
```

```python
import functools
import math

import jax
import jax.numpy as jnp
from jax import lax
from jax.experimental import pallas as pl
from jax.experimental.pallas import tpu as pltpu
from jax.sharding import PartitionSpec as P

BLK = 128
F32 = jnp.float32
BF16 = jnp.bfloat16
MESH = pl.DeviceIdType.MESH
CH = 8


def mm(a, b):
    return jnp.dot(a, b, preferred_element_type=F32)


def sig(x):
    return 0.5 * jnp.tanh(0.5 * x) + 0.5


def cell_update(gates, old, n):
    in_gate = sig(gates[:n])
    forget = sig(gates[n : 2 * n])
    cand = jnp.tanh(gates[2 * n : 3 * n])
    out_gate = sig(gates[3 * n :])
    fresh = forget * old.astype(F32) + in_gate * cand
    return (out_gate * jnp.tanh(fresh)).astype(BF16), fresh.astype(BF16)


def split3(x):
    hi = x.astype(BF16)
    rest = x - hi.astype(F32)
    mid = rest.astype(BF16)
    return hi, mid, (rest - mid.astype(F32)).astype(BF16)


def kernel(
    D,
    obs_h,
    nz_h,
    wh_h,
    wl_h,
    wf_h,
    bias_h,
    wp_h,
    we_h,
    weh_h,
    bs_h,
    off_h,
    fl_h,
    h4,
    lse_all,
    used_o,
    wh,
    wlf,
    wf,
    tpose,
    bias,
    wp,
    we,
    weh,
    obs,
    obs_pad,
    nz,
    off,
    bs,
    fl,
    rx,
    x0,
    x0_far,
    x1_far,
    g1,
    ga,
    gb,
    gc,
    hz,
    cz,
    h1,
    c1,
    hc,
    h2,
    c2,
    h3,
    c3,
    lse_row,
    wsem,
    lsem,
    ssem,
    rsem,
    as_sem,
    ar_sem,
    near_sem,
):
    H = wh.shape[3]
    Z = we.shape[1]
    X = we.shape[0]
    HC = H // CH
    me = lax.axis_index("dom")
    right = lax.rem(me + 1, D)
    left = lax.rem(me + D - 1, D)

    def signal(sem, dev, there):
        @pl.when(there)
        def _():
            pl.semaphore_signal(sem, inc=1, device_id={"dom": dev}, device_id_type=MESH)

    def partners(dist):
        return (
            (lax.rem(me + dist, D), me + dist < D),
            (lax.rem(me + D - dist, D), me >= dist),
        )

    def count(dist):
        return sum(jnp.where(there, 1, 0) for _, there in partners(dist))

    barrier = pltpu.get_barrier_semaphore()
    for dev, there in partners(1):
        signal(barrier, dev, there)

    def near_signal(i):
        for dev, there in partners(2**i):
            signal(near_sem.at[i], dev, there)

    def near_wait(i):
        pl.semaphore_wait(near_sem.at[i], count(2**i))

    small = []

    def fetch(src, dst):
        cp = pltpu.make_async_copy(src, dst, lsem.at[len(small)])
        cp.start()
        small.append(cp)
        return cp

    cp_n01 = fetch(nz_h.at[pl.ds(0, 2)], nz.at[pl.ds(0, 2)])
    cp_wf = fetch(wf_h, wf)
    cp_bias = fetch(bias_h, bias)
    cp_obs = fetch(obs_h, obs)
    cp_off = fetch(off_h, off)
    cp_bs = fetch(bs_h, bs)
    cp_fl = fetch(fl_h, fl)

    wcp = [
        (
            pltpu.make_async_copy(wh_h.at[:, c], wh.at[c], wsem.at[0, c]),
            pltpu.make_async_copy(wl_h.at[:, c], wlf.at[c, :, :, pl.ds(0, Z)], wsem.at[1, c]),
        )
        for c in range(CH)
    ]
    def start_weights(c, n):
        for pair in wcp[c : c + n]:
            for cp in pair:
                cp.start(priority=1)

    start_weights(0, 2)
    cp_wp = fetch(wp_h, wp)
    cp_n23 = fetch(nz_h.at[pl.ds(2, 2)], nz.at[pl.ds(2, 2)])
    cp_we = fetch(we_h, we)
    cp_weh = fetch(weh_h, weh)

    def link(side, k):
        src, dst = (
            (nz.at[0], rx.at[side, 0]),
            (nz.at[1], rx.at[side, 1]),
            (nz_h.at[2], rx.at[side, 2]),
            (x0.at[side], x0_far.at[side]),
            (rx.at[side, 1], x1_far.at[side]),
        )[k]
        return pltpu.make_async_remote_copy(
            src_ref=src,
            dst_ref=dst,
            send_sem=ssem.at[side, max(k - 2, 0)],
            recv_sem=rsem.at[side, k],
            device_id={"dom": lax.rem(me + 1 - 2 * side + D, D)},
            device_id_type=MESH,
        )

    def within(place):
        return jnp.logical_and(place >= 0, place < D)

    def step_of(side):
        return 1 - 2 * side

    def sends(side, k):
        ahead = within(me + step_of(side))
        return ahead if k < 3 else jnp.logical_and(ahead, within(me - step_of(side)))

    def send(side, k):
        @pl.when(sends(side, k))
        def _():
            link(side, k).start()

    def arrived(k, sides=(0, 1)):
        for side in sides:

            @pl.when(within(me - (1 if k < 3 else 2) * step_of(side)))
            def _():
                link(side, k).wait_recv()

    def all_sent():
        for side in range(2):

            @pl.when(sends(side, 0))
            def _():
                noise = pl.ds(0, 3)
                pltpu.make_async_remote_copy(
                    src_ref=nz_h.at[noise],
                    dst_ref=rx.at[side, noise],
                    send_sem=ssem.at[side, 0],
                    recv_sem=rsem.at[side, 0],
                    device_id={"dom": lax.rem(me + step_of(side) + D, D)},
                    device_id_type=MESH,
                ).wait_send()

            @pl.when(sends(side, 3))
            def _():
                link(side, 3).wait_send()
                link(side, 4).wait_send()

    hz[...] = jnp.zeros_like(hz)
    cz[...] = jnp.zeros_like(cz)
    obs_pad[...] = jnp.zeros_like(obs_pad)
    tpose[X // 16 * 16 :, :] = jnp.zeros((BLK - X // 16 * 16, tpose.shape[1]), BF16)

    start_weights(2, 6)
    cp_bs.wait()
    cp_fl.wait()
    cp_off.wait()
    cp_obs.wait()
    f0, f1, f2 = fl[0] == 1, fl[1] == 1, fl[2] == 1

    around = range(-2, 3)
    place = [lax.rem(me + d + D, D) for d in around]

    def src(t, k, f):
        found = bs[t, place[2]]
        for d, p in zip(around, place):
            found = jnp.where(k - me == d, bs[t, p], found)
        return jnp.where(f, found, k)

    lane = lax.broadcasted_iota(jnp.int32, (1, BLK), 1).astype(F32)
    sub_i = lax.broadcasted_iota(jnp.int32, (BLK, BLK), 0)
    sub = sub_i.astype(F32)

    def flag_mask(f, shape):
        return jnp.broadcast_to(f.astype(jnp.int32), shape) > 0

    def offs(t, k, f):
        away = jnp.broadcast_to(k - me, (1, BLK))
        row = lane
        for d, p in zip(around, place):
            there = off[pl.ds(t, 1), pl.ds(pl.multiple_of(p * BLK, BLK), BLK)].astype(F32)
            row = jnp.where(jnp.logical_and(flag_mask(f, (1, BLK)), away == d), there, row)
        return row

    def onehot(row):
        return jnp.where(sub == row, 1.0, 0.0).astype(BF16)

    def comp(row, hot):
        return mm(jnp.broadcast_to(row, (16, BLK)).astype(BF16), hot)[:1]

    k2 = src(2, me, f2)
    k1 = src(1, k2, f1)
    s1 = src(1, me, f1)
    s0 = src(0, me, f0)
    o0 = src(0, s1, f0)
    k0 = src(0, k1, f0)
    hot_q = onehot(offs(2, me, f2))
    hot_r = onehot(comp(offs(1, k2, f1), hot_q))
    hot_s = onehot(comp(offs(0, k1, f0), hot_r))
    hot_o1 = onehot(offs(1, me, f1))
    hot_o0 = onehot(comp(offs(0, s1, f0), hot_o1))
    hot_c0 = onehot(offs(0, me, f0))
    def pick(t, k):
        d = jnp.broadcast_to(k - me, (Z, BLK))
        out = jnp.where(d < 0, rx[0, t], jnp.where(d > 0, rx[1, t], nz[t]))
        if t != 1:
            return out
        return jnp.where(d == -2, x1_far[0], jnp.where(d == 2, x1_far[1], out))

    def latent_0(k, hot, far=True):
        lat = mean0 + std0 * pick(0, k)
        if far:
            d = jnp.broadcast_to(k - me, (Z, BLK))
            lat = jnp.where(d == -2, x0_far[0].astype(F32), lat)
            lat = jnp.where(d == 2, x0_far[1].astype(F32), lat)
        return mm(lat.astype(BF16), hot).astype(BF16)

    def gather3(x, hot):
        hi, mid, lo = split3(x)
        out = mm(jnp.concatenate([hi, mid, lo], axis=0), hot)
        return out[:BLK] + out[BLK : 2 * BLK] + out[2 * BLK :]

    steps = obs.shape[0] - 1
    obs_pad[0 : steps + 1, 0:X] = obs[...].astype(F32)
    obs_t = jnp.transpose(obs_pad[...])

    def frame_col(t):
        return jnp.broadcast_to(obs_t[:, t : t + 1], (BLK, BLK))

    ones = jnp.logical_and(sub_i >= 96, sub_i < 99)
    tails = [jnp.where(ones, 1.0, frame_col(t)).astype(BF16) for t in range(steps)]

    cp_wf.wait()
    cp_bias.wait()
    tpose[0:X, :] = wf[...]
    hi, mid, lo = (p.astype(F32) for p in split3(bias[...]))
    r16 = lax.broadcasted_iota(jnp.int32, (16, bias.shape[1]), 0)
    tpose[96:112, :] = jnp.where(
        r16 == 0, hi, jnp.where(r16 == 1, mid, jnp.where(r16 == 2, lo, 0.0))
    ).astype(BF16)
    for c in range(CH):
        for g in range(4):
            for i in range(0, HC, BLK):
                rows = g * H + c * HC + i
                wlf[c, g, i : i + BLK, Z : Z + BLK] = jnp.transpose(
                    tpose[:, rows : rows + BLK]
                )

    pl.semaphore_wait(barrier, count(1))
    cp_n01.wait()
    for t in range(3):
        for side in range(2):
            send(side, t)
    near_signal(0)

    def run_layer(gates, elem, hooks={}):
        bufs = (ga, gb)
        for c in range(CH):
            hooks.get(c, lambda: None)()
            val = gates(c)
            bufs[c % 2][:, : val.shape[1]] = val
            if c:
                elem(c - 1, bufs[(c - 1) % 2])
        elem(CH - 1, bufs[(CH - 1) % 2])

    def elem_of(n, old, h_out, c_out):
        def elem(c, buf):
            rows = slice(c * HC, (c + 1) * HC)
            h, s = cell_update(buf[:, :n], old[rows, :n], HC)
            h_out[rows, :n] = h
            if c_out is not None:
                c_out[rows, :n] = s

        return elem

    def moments(h):
        return mm(wp[:Z, :], h), jnp.exp(0.5 * jnp.tanh(mm(wp[Z:, :], h)))

    def increment(t, lat, h):
        pred = mm(we[...], lat) + mm(weh[...], h)
        target = frame_col(t + 1)[:X]
        return jnp.sum(pred * (target - 0.5 * pred), axis=0, keepdims=True)

    lat_tail0 = jnp.concatenate([jnp.zeros((Z, BLK), BF16), tails[0]], axis=0)

    def halves(c, first, tail=None):
        out = []
        for g in (0, 2):
            rows = slice(g * HC, (g + 2) * HC)
            val = first(g, rows)
            if tail is not None:
                val = val + mm(wlf[c, g : g + 2].reshape(2 * HC, Z + BLK), tail)
            out.append(val)
        return jnp.concatenate(out, axis=0)

    def product(c, state, tail=None):
        def first(g, rows):
            return mm(wh[c, g : g + 2].reshape(2 * HC, H), state)

        return halves(c, first, tail)

    def with_tail(c, ref, tail, wide=False):
        def first(g, rows):
            part = ref[c, rows, :]
            return jnp.concatenate([part, part], axis=1) if wide else part

        return halves(c, first, tail)

    def weights_here(c, n):
        for pair in wcp[c : c + n]:
            for cp in pair:
                cp.wait()

    def third():
        weights_here(4, 4)
        near_wait(0)
        near_signal(1)
        cp_wp.wait()
        cp_n23.wait()
        cp_we.wait()
        cp_weh.wait()

    run_layer(
        lambda c: product(c, hz[...], lat_tail0),
        elem_of(BLK, cz, h1, c1),
        {0: lambda: weights_here(0, 2), 2: lambda: weights_here(2, 2), 4: third},
    )
    mean0, std0 = moments(h1[...])

    def relay_0(side):
        arrived(0, (side,))
        x0[side] = (mean0 + std0 * rx[side, 0]).astype(BF16)
        send(side, 3)

    first = jnp.where(lax.rem(me, 4) == 0, 1, 0)
    relay_0(first)
    inner = jnp.logical_or(lax.rem(me, 4) == 1, lax.rem(me, 4) == 2)

    @pl.when(inner)
    def _():
        relay_0(1 - first)

    for c in range(2):
        g1[c] = product(c, h1[...])

    @pl.when(jnp.logical_not(inner))
    def _():
        relay_0(1 - first)

    near_wait(1)
    near_signal(2)
    lat_c = latent_0(s0, hot_c0, False)
    tail_c = jnp.concatenate([lat_c, tails[1]], axis=0)
    lw0 = increment(0, (mean0 + std0 * nz[0]).astype(BF16), h1[...])

    def gates_c(c):
        if c > 1:
            g1[c] = product(c, h1[...])
        return with_tail(c, g1, tail_c)

    def relay_1():
        arrived(1)
        send(0, 4)
        send(1, 4)

    run_layer(gates_c, elem_of(BLK, c1, hc, None), {4: relay_1})
    near_wait(2)
    arrived(3)
    near_signal(3)

    lat_o = latent_0(o0, hot_o0)
    lat_l = latent_0(k0, hot_s)
    tail_ol = jnp.concatenate(
        [
            jnp.concatenate([lat_o, lat_l], axis=1),
            jnp.concatenate([tails[1], tails[1]], axis=1),
        ],
        axis=0,
    )

    def gates1(c):
        return with_tail(c, g1, tail_ol, True)

    def elem1(c, buf):
        rows = slice(c * HC, (c + 1) * HC)
        old = c1[rows, :]
        h, s = cell_update(buf[...], jnp.concatenate([old, old], axis=1), HC)
        h2[rows, :] = h
        c2[rows, :] = s

    run_layer(gates1, elem1)
    m1, sd1 = moments(h2[...])
    early, late = 2, 4
    for c in range(early):
        gc[c] = product(c, h2[...])
    mean_c, std_c = moments(hc[...])
    inc_c = increment(1, (mean_c + std_c * nz[1]).astype(BF16), hc[...])
    lw1 = jnp.where(flag_mask(f0, (1, BLK)), 0.0, lw0) + inc_c
    near_wait(3)
    arrived(4)
    arrived(2)
    near_signal(4)
    n1_o = gather3(pick(1, s1), hot_o1)
    n1_l = gather3(pick(1, k1), hot_r)
    for c in range(early, late):
        gc[c] = product(c, h2[...])
    lat1 = (m1 + sd1 * jnp.concatenate([n1_o, n1_l], axis=1)).astype(BF16)

    tail2 = jnp.concatenate(
        [lat1, jnp.concatenate([tails[2], tails[2]], axis=1)], axis=0
    )

    def gates2(c):
        if c < late:
            return with_tail(c, gc, tail2)
        return product(c, h2[...], tail2)

    run_layer(gates2, elem_of(2 * BLK, c2, h3, c3))
    m2, sd2 = moments(h3[...])
    for c in range(2):
        g1[c] = product(c, h3[:, BLK:])
    n2_l = gather3(pick(2, k2), hot_q)
    lat2 = (m2 + sd2 * jnp.concatenate([nz[2], n2_l], axis=1)).astype(BF16)
    tail3 = jnp.concatenate([lat2[:, BLK:], tails[3]], axis=0)

    def gates3(c):
        if c < 2:
            return with_tail(c, g1, tail3)
        return product(c, h3[:, BLK:], tail3)

    def elem3(c, buf):
        rows = slice(c * HC, (c + 1) * HC)
        h, _ = cell_update(buf[:, :BLK], c3[rows, BLK:], HC)
        h4[rows, :] = h

    run_layer(gates3, elem3)
    inc2 = increment(2, lat2[:, :BLK], h3[:, :BLK])
    lw2 = jnp.where(flag_mask(f1, (1, BLK)), 0.0, lw1) + inc2
    m3, sd3 = moments(h4[...])
    lat3 = (m3 + sd3 * nz[3]).astype(BF16)
    lw3 = jnp.where(flag_mask(f2, (1, BLK)), 0.0, lw2) + increment(3, lat3, h4[...])

    def lse(lw):
        peak = jnp.max(lw, axis=1, keepdims=True)
        return peak + jnp.log(jnp.sum(jnp.exp(lw - peak), axis=1, keepdims=True))

    lane_i = lax.broadcasted_iota(jnp.int32, (1, BLK), 1)
    row = jnp.zeros((1, BLK), F32)
    for t, lw in enumerate((lw0, lw1, lw2, lw3)):
        row = jnp.where(lane_i == t, lse(lw), row)
    lse_row[...] = row
    lse_all[pl.ds(me, 1)] = row[None]
    used = lane_i == steps - 1
    for t, f in enumerate((f0, f1, f2)):
        used = jnp.logical_or(used, jnp.logical_and(lane_i == t, flag_mask(f, (1, BLK))))
    used_o[...] = jnp.where(used, 1.0, 0.0)
    near_wait(4)
    for d in range(1, D):
        pltpu.make_async_remote_copy(
            src_ref=lse_row,
            dst_ref=lse_all.at[me],
            send_sem=as_sem,
            recv_sem=ar_sem,
            device_id={"dom": lax.rem(me + d, D)},
            device_id_type=MESH,
        ).start()
    all_sent()
    others = lse_all.at[pl.ds(0, D - 1)]
    every = pltpu.make_async_remote_copy(
        src_ref=others,
        dst_ref=others,
        send_sem=as_sem,
        recv_sem=ar_sem,
        device_id={"dom": right},
        device_id_type=MESH,
    )
    every.wait_recv()
    every.wait_send()


def finish(h_ref, lse_all, used, hid_o, bnd_o, bnd, sem):
    out_cp = pltpu.make_async_copy(h_ref, hid_o, sem.at[0])
    out_cp.start()
    every = lse_all[...]
    peak = jnp.max(every, axis=0)
    total = jnp.log(jnp.sum(jnp.exp(every - peak[None]), axis=0))
    level = peak + total - math.log(every.shape[0] * BLK)
    bnd[...] = jnp.sum(jnp.where(used[...] > 0, level, 0.0), axis=1, keepdims=True)
    bnd_cp = pltpu.make_async_copy(bnd, bnd_o, sem.at[1])
    bnd_cp.start()
    out_cp.wait()
    bnd_cp.wait()


def body(
    observed,
    latent_noise,
    w_hidden,
    w_latent,
    w_frame,
    gate_bias,
    w_prior,
    w_emit,
    w_emit_hidden,
    block_source,
    inner_offset,
    resample_flags,
):
    D = lax.axis_size("dom")
    steps, Z, n = latent_noise.shape
    H = w_hidden.shape[1]
    X = w_emit.shape[0]
    G = 4 * H // CH
    V = pltpu.VMEM
    DMA = pltpu.SemaphoreType.DMA
    pinned = [
        pltpu.with_memory_space_constraint(x, pltpu.HBM)
        for x in (
            observed,
            latent_noise,
            w_hidden.reshape(4, CH, H // CH, H),
            w_latent.reshape(4, CH, H // CH, Z),
            w_frame,
            gate_bias.reshape(1, -1),
            w_prior,
            w_emit,
            w_emit_hidden,
            block_source,
            inner_offset,
            resample_flags,
        )
    ]
    last_hidden, lse_all, used = pl.pallas_call(
        functools.partial(kernel, D),
        out_shape=(
            jax.ShapeDtypeStruct((H, n), BF16),
            jax.ShapeDtypeStruct((D, 1, BLK), F32),
            jax.ShapeDtypeStruct((1, BLK), F32),
        ),
        in_specs=[pl.BlockSpec(memory_space=pltpu.HBM)] * 12,
        out_specs=(pl.BlockSpec(memory_space=pltpu.VMEM),) * 3,
        scratch_shapes=[
            V((CH, 4, H // CH, H), BF16),
            V((CH, 4, H // CH, Z + BLK), BF16),
            V((X, 4 * H), BF16),
            V((BLK, 4 * H), BF16),
            V((1, 4 * H), F32),
            V((2 * Z, H), BF16),
            V((X, Z), BF16),
            V((X, H), BF16),
            V((steps + 1, X), BF16),
            V((BLK, BLK), F32),
            V((steps, Z, n), F32),
            V(inner_offset.shape, jnp.int32),
            pltpu.SMEM(block_source.shape, jnp.int32),
            pltpu.SMEM(resample_flags.shape, jnp.int32),
            V((2, 3, Z, n), F32),
            V((2, Z, n), BF16),
            V((2, Z, n), BF16),
            V((2, Z, n), F32),
            V((CH, G, n), F32),
            V((G, 2 * n), F32),
            V((G, 2 * n), F32),
            V((CH // 2 + 2, G, 2 * n), F32),
            V((H, n), BF16),
            V((H, n), BF16),
            V((H, n), BF16),
            V((H, n), BF16),
            V((H, n), BF16),
            V((H, 2 * n), BF16),
            V((H, 2 * n), BF16),
            V((H, 2 * n), BF16),
            V((H, 2 * n), BF16),
            V((1, BLK), F32),
            DMA((2, CH)),
            DMA((11,)),
            DMA((2, 3)),
            DMA((2, 5)),
            DMA,
            DMA,
            pltpu.SemaphoreType.REGULAR((5,)),
        ],
        compiler_params=pltpu.CompilerParams(
            collective_id=0, has_side_effects=True, vmem_limit_bytes=32 * 2**20
        ),
        name="filter_steps",
    )(*pinned)
    hidden, bound = pl.pallas_call(
        finish,
        out_shape=(
            jax.ShapeDtypeStruct((H, n), BF16),
            jax.ShapeDtypeStruct((1, 1), F32),
        ),
        in_specs=[pl.BlockSpec(memory_space=pltpu.VMEM)] * 3,
        out_specs=(pl.BlockSpec(memory_space=pl.ANY),) * 2,
        scratch_shapes=[V((1, 1), F32), DMA((2,))],
        compiler_params=pltpu.CompilerParams(vmem_limit_bytes=2 * 2**20),
        name="finish",
    )(last_hidden, lse_all, used)
    return hidden, bound.reshape(1)


def solution(mesh):
    in_specs = (
        P("seq", None),
        P(None, None, ("seq", "dom")),
        P(),
        P(),
        P(),
        P(),
        P(),
        P(),
        P(),
        P("seq", None),
        P("seq", None),
        P(),
    )
    out_specs = (P(None, ("seq", "dom")), P("seq"))
    return jax.shard_map(body, mesh=mesh, in_specs=in_specs, out_specs=out_specs, check_vma=False)
```
